32 devices in a mesh: ens: 4 (over x, core), elem: 8 (over z, y).
Axes of the slice: x: 2, y: 2, z: 4, core: 2. Of those that a mesh axis runs over, the one named last changes fastest.
Arguments:
- scalars: float32 [8, 512, 1024], P('ens', None, 'elem'), parts along dimension 0, may hold values from -6 to 6
- transport: float32 [3, 512, 1024], P(None, None, 'elem'), may hold values from -6 to 6
- mass: float32 [512, 1024], P(None, 'elem'), may hold values from 0.5 to 2
- element_order: int32 [8, 128], P('elem'), may hold values from 0 to 127, each once within a row
Outputs:
- advected: float32 [8, 512, 1024], P('ens', None, 'elem'), parts along dimension 0
The draws below stay inside these ranges and needn't reach their ends.
There are 4 independent parts, one for each index of `ens`. The reference program is written for one: setup_inputs(seed, part) draws one part's arguments, and reference() takes and returns one part's arrays. A program takes and returns all parts, laid end to end along the dimension named above; an argument that names none is the same for every part. Nothing has to cross between parts.
Inputs may be any that keep to these rules, and one draw needn't show every extreme that they name: `element_order`: each row is a permutation of the device's slots.
All inputs are finite; a program needn't handle non-finite values.
Results may differ from the reference program's by a relative error of at most 0.0001.
Values sent between devices are 32-bit elements; how exact they have to be, the bound alone decides.
A program may use at most 64 MiB of HBM per device.

```python
import math
import jax
import jax.numpy as jnp
import numpy as np
from jax import lax

ORDER = 7
NODES = 512
MEMB = 2
SUBSTEPS = 2
EX = 1
EY = 8
EZ = 16
E_DEV = 128
ELEMS = 1024
N_ELEM = 8


def block_levels(own_key, shape, cuts, smallest, largest):
    level, own = 1.0, jax.random.fold_in(own_key, 6)
    for dim, blocks in cuts:
        heights = jnp.exp(jax.random.uniform(jax.random.fold_in(own, dim), (blocks,), jnp.float32, smallest / len(cuts), largest / len(cuts)))
        level = level * jnp.repeat(heights, shape[dim] // blocks).reshape([-1 if axis == dim else 1 for axis in range(len(shape))])
    return level


def bell_draw(own_key, shape, deviation, most, split=(), held_as=jnp.bfloat16):
    result = deviation * jax.random.normal(own_key, shape, jnp.float32)
    if split:
        result = result * block_levels(own_key, shape, split, -0.22, 0.18)
    return jnp.clip(result, -most, most).astype(held_as)


def setup_inputs(seed: int = 0, part: int = 0) -> dict:
    key_list = jax.random.split(jax.random.key(seed), 5)
    part_keys = jax.random.split(jax.random.fold_in(key_list[4], part), 5)
    scalars = bell_draw(part_keys[0], (MEMB, NODES, ELEMS), 1.0, 6.0, ((2, 8),), jnp.float32)
    transport = bell_draw(key_list[1], (3, NODES, ELEMS), 1.0, 6.0, ((2, 8),), jnp.float32)
    mass = jnp.clip(jnp.exp(math.log(2.0) - 1.3862944 * jax.random.uniform(key_list[2], (NODES, ELEMS), jnp.float32) ** block_levels(key_list[2], (NODES, ELEMS), ((1, 8),), -0.2, 0.2)), 0.5, 2.0)
    element_order = jax.vmap(lambda own: jax.random.permutation(own, E_DEV))(jax.random.split(key_list[3], N_ELEM)).reshape((N_ELEM, E_DEV)).astype(jnp.int32)
    return {"scalars": scalars, "transport": transport, "mass": mass, "element_order": element_order}


time_step = 0.015


def legendre_table(points, degree):
    table = np.zeros((points.shape[0], degree + 1))
    table[:, 0] = 1.0
    table[:, 1] = points
    for level in range(2, degree + 1):
        table[:, level] = ((2 * level - 1) * points * table[:, level - 1] - (level - 1) * table[:, level - 2]) / level
    return table


def gll_derivative(degree):
    extent = degree + 1
    points = np.cos(np.pi * np.arange(extent) / degree)
    for sweep in range(60):
        table = legendre_table(points, degree)
        points = points - (points * table[:, degree] - table[:, degree - 1]) / (extent * table[:, degree])
    points = points[::-1].copy()
    values = legendre_table(points, degree)[:, degree]
    matrix = np.zeros((extent, extent))
    for target in range(extent):
        for source in range(extent):
            if target != source:
                matrix[target, source] = values[target] / (values[source] * (points[target] - points[source]))
    matrix[0, 0] = -degree * (degree + 1) / 4.0
    matrix[extent - 1, extent - 1] = degree * (degree + 1) / 4.0
    return matrix


def assemble(field):
    last = ORDER
    upper = field[..., last, :, :, :, :, :] + jnp.roll(field[..., 0, :, :, :, :, :], -1, axis=-3)
    field = field.at[..., last, :, :, :, :, :].set(upper).at[..., 0, :, :, :, :, :].set(jnp.roll(upper, 1, axis=-3))
    upper = field[..., last, :, :, :, :] + jnp.roll(field[..., 0, :, :, :, :], -1, axis=-2)
    field = field.at[..., last, :, :, :, :].set(upper).at[..., 0, :, :, :, :].set(jnp.roll(upper, 1, axis=-2))
    upper = field[..., last, :, :, :] + jnp.roll(field[..., 0, :, :, :], -1, axis=-1)
    field = field.at[..., last, :, :, :].set(upper).at[..., 0, :, :, :].set(jnp.roll(upper, 1, axis=-1))
    return field


def reference(scalars, transport, mass, element_order):
    extent = ORDER + 1
    derivative = jnp.asarray(gll_derivative(ORDER), jnp.float32)
    highest = lax.Precision.HIGHEST
    position = (jnp.arange(N_ELEM, dtype=jnp.int32)[:, None] * E_DEV + element_order.astype(jnp.int32)).reshape(-1)

    def to_brick(values):
        placed = jnp.zeros_like(values).at[..., position].set(values)
        return placed.reshape(values.shape[:-2] + (extent, extent, extent, EX * N_ELEM, EY, EZ))

    field = to_brick(scalars)
    velocity = to_brick(transport)
    weights = to_brick(mass)
    summed = assemble(jnp.concatenate([weights[None] * field, weights[None]], axis=0))
    total_mass = summed[MEMB]
    field = summed[:MEMB] / total_mass

    def tendency(values):
        grad_r = jnp.einsum('ai,...ijkxyz->...ajkxyz', derivative, values, precision=highest)
        grad_s = jnp.einsum('bj,...ijkxyz->...ibkxyz', derivative, values, precision=highest)
        grad_t = jnp.einsum('ck,...ijkxyz->...ijcxyz', derivative, values, precision=highest)
        weighted = velocity[0] * grad_r + velocity[1] * grad_s + velocity[2] * grad_t
        return -assemble(weighted) / total_mass

    for substep in range(SUBSTEPS):
        first_k = tendency(field)
        second_k = tendency(field + 0.5 * time_step * first_k)
        third_k = tendency(field + 0.5 * time_step * second_k)
        fourth_k = tendency(field + time_step * third_k)
        field = field + (time_step / 6.0) * (first_k + 2.0 * second_k + 2.0 * third_k + fourth_k)
    flat = field.reshape(MEMB, NODES, ELEMS)
    return flat[..., position]
```

```python
import functools

import jax
import jax.numpy as jnp
import numpy as np
from jax import lax
from jax.experimental import pallas as pl
from jax.experimental.pallas import tpu as pltpu
from jax.sharding import PartitionSpec as P

ORDER = 7
SUBSTEPS = 2
EX = 1
EY = 8
EZ = 16
EXTENT = ORDER + 1
PLANE = EXTENT * EXTENT
NODES = EXTENT * PLANE
MESH = pl.DeviceIdType.MESH
NEAR, FAR, NEXT = 0, 1, 2


time_step = 0.015


def legendre_table(points, degree):
    table = np.zeros((points.shape[0], degree + 1))
    table[:, 0] = 1.0
    table[:, 1] = points
    for level in range(2, degree + 1):
        table[:, level] = (
            (2 * level - 1) * points * table[:, level - 1] - (level - 1) * table[:, level - 2]
        ) / level
    return table


def gll_derivative(degree):
    extent = degree + 1
    points = np.cos(np.pi * np.arange(extent) / degree)
    for sweep in range(60):
        table = legendre_table(points, degree)
        points = points - (points * table[:, degree] - table[:, degree - 1]) / (
            extent * table[:, degree]
        )
    points = points[::-1].copy()
    values = legendre_table(points, degree)[:, degree]
    matrix = np.zeros((extent, extent))
    for target in range(extent):
        for source in range(extent):
            if target != source:
                matrix[target, source] = values[target] / (
                    values[source] * (points[target] - points[source])
                )
    matrix[0, 0] = -degree * (degree + 1) / 4.0
    matrix[extent - 1, extent - 1] = degree * (degree + 1) / 4.0
    return matrix


def split_matrix():
    derivative = gll_derivative(ORDER).astype(np.float32)
    eye = np.eye(EXTENT, dtype=np.float32)
    full = np.concatenate([np.kron(derivative, eye), np.kron(eye, derivative)], axis=0)
    high = full.astype(jnp.bfloat16)
    low = (full - high.astype(np.float32)).astype(jnp.bfloat16)
    return np.concatenate([high, high, low], axis=1)


def halves(values):
    high = values.astype(jnp.bfloat16)
    low = (values - high.astype(jnp.float32)).astype(jnp.bfloat16)
    return high, low


def lane_forward(values, stride, length):
    total = values.shape[-1]
    near = pltpu.roll(values, total - stride, 1)
    if stride * length == total:
        return near
    coords = lax.broadcasted_iota(jnp.int32, values.shape, 1) // stride % length
    return jnp.where(coords < length - 1, near, pltpu.roll(values, stride * (length - 1), 1))


def lane_backward(values, stride, length):
    total = values.shape[-1]
    near = pltpu.roll(values, stride, 1)
    if stride * length == total:
        return near
    coords = lax.broadcasted_iota(jnp.int32, values.shape, 1) // stride % length
    return jnp.where(coords > 0, near, pltpu.roll(values, total - stride * (length - 1), 1))


def store_assembled(ref, row, values):
    low, high = values[:EXTENT], values[PLANE - EXTENT :]
    ref[row : row + EXTENT] = low + lane_backward(high, EZ, EY)
    ref[row + EXTENT : row + PLANE - EXTENT] = values[EXTENT : PLANE - EXTENT]
    ref[row + PLANE - EXTENT : row + PLANE] = high + lane_forward(low, EZ, EY)
    first = pl.ds(row, EXTENT, stride=EXTENT)
    last = pl.ds(row + ORDER, EXTENT, stride=EXTENT)
    k_low = ref[first, :]
    k_high = ref[last, :]
    ref[first, :] = k_low + lane_backward(k_high, 1, EZ)
    ref[last, :] = k_high + lane_forward(k_low, 1, EZ)


def store_lower(ref, row, values):
    low, high = values[:EXTENT], values[PLANE - EXTENT :]
    ref[row : row + EXTENT] = low + lane_backward(high, EZ, EY)
    ref[row + EXTENT : row + PLANE] = values[EXTENT:]
    first = pl.ds(row, EXTENT, stride=EXTENT)
    k_high = ref[pl.ds(row + ORDER, EXTENT, stride=EXTENT), :]
    ref[first, :] = ref[first, :] + lane_backward(k_high, 1, EZ)


def pack(source, row, target):
    for j in range(ORDER):
        target[j * ORDER : j * ORDER + EXTENT] = source[row + j * EXTENT : row + (j + 1) * EXTENT]


def add_packed(ref, row, packed):
    for j in range(ORDER):
        part = slice(row + j * EXTENT, row + (j + 1) * EXTENT)
        ref[part] = ref[part] + packed[j * ORDER : j * ORDER + EXTENT]
    k_low = ref[pl.ds(row, EXTENT, stride=EXTENT), :]
    ref[pl.ds(row + ORDER, EXTENT, stride=EXTENT), :] = lane_forward(k_low, 1, EZ)
    ref[row + PLANE - EXTENT : row + PLANE] = lane_forward(ref[row : row + EXTENT], EZ, EY)


def expand_packed(ref, row, packed, scale):
    for j in range(ORDER):
        ref[row + j * EXTENT : row + (j + 1) * EXTENT] = (
            scale * packed[j * ORDER : j * ORDER + EXTENT]
        )
    spread_lower(ref, row)


def spread_lower(ref, row):
    k_low = ref[pl.ds(row, EXTENT, stride=EXTENT), :]
    ref[pl.ds(row + ORDER, EXTENT, stride=EXTENT), :] = lane_forward(k_low, 1, EZ)
    ref[row + PLANE - EXTENT : row + PLANE] = lane_forward(ref[row : row + EXTENT], EZ, EY)


def kernel(
    count, members, scalars, transport, mass, order, matrix, state,
    speed, middle, ahead, work, raw, near, far, joint, cross, beyond,
    mass_send, mass_recv, mass_send_sem, mass_recv_sem,
    coef_send, coef_recv, coef_send_sem, coef_recv_sem,
    send, recv, send_sem, recv_sem,
):
    me = lax.axis_index("elem")

    def shifted(distance):
        return lax.rem(me + distance + count, count)

    barrier = pltpu.get_barrier_semaphore()
    for distance in (-2, -1, 1, 2):
        pl.semaphore_signal(
            barrier, inc=1, device_id={"elem": shifted(distance)}, device_id_type=MESH
        )

    elements = order.shape[-1]
    lanes = lax.broadcasted_iota(jnp.int32, (elements, elements), 0)
    chosen = jnp.where(order[...] == lanes, 1.0, 0.0).astype(jnp.bfloat16)
    to_brick_matrix = jnp.concatenate([chosen, chosen], axis=1)

    def to_brick(values):
        return lax.dot_general(
            jnp.concatenate(halves(values), axis=1),
            to_brick_matrix,
            (((1,), (1,)), ((), ())),
            preferred_element_type=jnp.float32,
        )

    first_side = 1 - lax.rem(me, 2)
    sides = (first_side, 1 - first_side)
    ends = (ORDER, 0)

    def target(side, distance):
        return {"elem": lax.rem(me + count + distance * (1 - 2 * side), count)}

    def mass_copies(m):
        return [
            pltpu.make_async_remote_copy(
                src_ref=mass_send.at[m, side, pl.ds(0, ORDER * ORDER)],
                dst_ref=mass_recv.at[m, side, pl.ds(0, ORDER * ORDER)],
                send_sem=mass_send_sem.at[m, side],
                recv_sem=mass_recv_sem.at[m, side],
                device_id=target(side, 1),
                device_id_type=MESH,
            )
            for side in sides
        ]

    def coef_copies():
        return [
            pltpu.make_async_remote_copy(
                src_ref=coef_send.at[side],
                dst_ref=coef_recv.at[side],
                send_sem=coef_send_sem.at[side],
                recv_sem=coef_recv_sem.at[side],
                device_id=target(side, 1),
                device_id_type=MESH,
            )
            for side in sides
        ]

    def face_copies(slot, m, kinds):
        return [
            pltpu.make_async_remote_copy(
                src_ref=send.at[slot, m, side, kind // 2, pl.ds(0, ORDER * ORDER)],
                dst_ref=recv.at[slot, m, side, kind, pl.ds(0, ORDER * ORDER)],
                send_sem=send_sem.at[slot, m, side, kind],
                recv_sem=recv_sem.at[slot, m, side, kind],
                device_id=target(side, 2 if kind == FAR else 1),
                device_id_type=MESH,
            )
            for side in sides
            for kind in kinds
        ]

    def row_of(m, i):
        return (m * EXTENT + i) * PLANE

    def rows_of(m, i):
        return slice(row_of(m, i), row_of(m, i) + PLANE)

    def plane_rows(i):
        return slice(i * PLANE, (i + 1) * PLANE)

    def block(values, place):
        return values[place * PLANE : (place + 1) * PLANE]

    def side_rows(m, side):
        return slice((m * 2 + side) * PLANE, (m * 2 + side + 1) * PLANE)

    outer = to_brick(
        jnp.concatenate(
            [mass[plane_rows(i), :] for i in ends]
            + [scalars[m, plane_rows(i), :] for m in range(members) for i in ends],
            axis=0,
        )
    )
    for side, i in enumerate(ends):
        store_lower(work, row_of(members, i), block(outer, side))
        pack(work, row_of(members, i), mass_send.at[members, side])
    for m in range(members):
        for side, i in enumerate(ends):
            store_lower(
                work, row_of(m, i), block(outer, side) * block(outer, 2 * (m + 1) + side)
            )
            pack(work, row_of(m, i), mass_send.at[m, side])
    pl.semaphore_wait(barrier, 4)
    for m in (members, *range(members)):
        for copy in mass_copies(m):
            copy.start()

    outer = to_brick(
        jnp.concatenate([transport[r, plane_rows(i), :] for r in range(3) for i in ends], axis=0)
    )
    for r in range(3):
        for side, i in enumerate(ends):
            speed[r, plane_rows(i), :] = block(outer, 2 * r + side)
            coef_send[side, r] = block(outer, 2 * r + side)
    for copy in coef_copies():
        copy.start()

    inner = slice(PLANE, NODES - PLANE)
    for r in range(3):
        speed[r, inner, :] = to_brick(transport[r, inner, :])
    middle[inner, :] = to_brick(mass[inner, :])
    for m in range(members):
        rows = slice(m * NODES + PLANE, (m + 1) * NODES - PLANE)
        ahead[rows, :] = to_brick(scalars[m, inner, :])
    for i in range(1, ORDER):
        weight = middle[plane_rows(i), :]
        store_assembled(work, row_of(members, i), weight)
        for m in range(members):
            store_assembled(work, row_of(m, i), weight * ahead[rows_of(m, i), :])

    def begin(m, i):
        state[0, rows_of(m, i), :] = work[rows_of(m, i), :] * work[rows_of(members, i), :]

    def scale(i):
        inverse = 1.0 / work[rows_of(members, i), :]
        work[rows_of(members, i), :] = inverse
        for r in range(3):
            speed[r, plane_rows(i), :] = speed[r, plane_rows(i), :] * (-time_step * inverse)

    for i in range(1, ORDER):
        scale(i)
        for m in range(members):
            begin(m, i)

    def take_masses(m):
        for copy in mass_copies(m):
            copy.wait()
        add_packed(work, row_of(m, 0), mass_recv.at[m, 0])
        add_packed(work, row_of(m, ORDER), mass_recv.at[m, 1])

    take_masses(members)
    scale(0)
    scale(ORDER)

    derivative = gll_derivative(ORDER)
    half = EXTENT // 2

    def inside_of(planes):
        stacked = []
        for values in planes:
            high, low = halves(values)
            stacked.append(jnp.concatenate([high, low, high], axis=0))
        return jnp.dot(
            matrix[...], jnp.concatenate(stacked, axis=1), preferred_element_type=jnp.float32
        )

    def pair(plane, a):
        even = odd = None
        for i in range(half):
            one, other = plane(i), plane(ORDER - i)
            plus = float(derivative[a, i] + derivative[a, ORDER - i]) * 0.5
            minus = float(derivative[a, i] - derivative[a, ORDER - i]) * 0.5
            even_term = plus * (one + other)
            odd_term = minus * (one - other)
            even = even_term if even is None else even + even_term
            odd = odd_term if odd is None else odd + odd_term
        inside = inside_of([plane(a), plane(ORDER - a)])
        for place, (i, across) in enumerate(((a, odd + even), (ORDER - a, odd - even))):
            columns = slice(place * elements, (place + 1) * elements)
            yield i, (
                speed[0, plane_rows(i), :] * across
                + speed[1, plane_rows(i), :] * inside[:PLANE, columns]
                + speed[2, plane_rows(i), :] * inside[PLANE:, columns]
            )

    def reaches(slot):
        return jnp.where(slot == 0, 0.25, 0.5), jnp.where(slot == 0, 1.0 / 3.0, 1.0)

    def first_faces(index, m):
        slot = lax.rem(index, 2)
        for i, value in pair(lambda n: state[slot, rows_of(m, n), :], 0):
            side = ends.index(i)
            store_lower(work, row_of(m, i), value)
            pack(work, row_of(m, i), send.at[slot, m, side, 0])
        for copy in face_copies(slot, m, (FAR, NEAR)):
            copy.start()

    def first_inner(index, m):
        slot = lax.rem(index, 2)
        reach, _ = reaches(slot)
        for i in ends:
            spread_lower(work, row_of(m, i))
            middle[rows_of(m, i), :] = state[0, rows_of(m, i), :] + reach * work[rows_of(m, i), :]
        for a in range(1, half):
            for i, value in pair(lambda n: state[slot, rows_of(m, n), :], a):
                store_assembled(work, row_of(m, i), value)
                middle[rows_of(m, i), :] = (
                    state[0, rows_of(m, i), :] + reach * work[rows_of(m, i), :]
                )
        for side, i in enumerate(ends):
            across = None
            for n in range(EXTENT):
                if n != i:
                    term = float(derivative[i, n]) * middle[rows_of(m, n), :]
                    across = term if across is None else across + term
            value = speed[0, plane_rows(i), :] * across
            raw[side_rows(m, side), :] = value
            store_lower(work, row_of(m, i), value)
            pack(work, row_of(m, i), send.at[slot, m, side, 1])
        for copy in face_copies(slot, m, (NEXT,)):
            copy.start()

    def second_ahead(index, m):
        _, reach = reaches(lax.rem(index, 2))
        for a in range(1, half):
            for i, value in pair(lambda n: middle[rows_of(m, n), :], a):
                store_assembled(work, row_of(m, i), value)
                ahead[rows_of(m, i), :] = (
                    state[0, rows_of(m, i), :] + reach * work[rows_of(m, i), :]
                )

    def second(index, m):
        slot = lax.rem(index, 2)
        reach, final_reach = reaches(slot)
        for copy in face_copies(slot, m, (NEAR, FAR, NEXT)):
            copy.wait()
        planes = (0, ORDER)
        for side, i in enumerate(planes):
            row = (m * 2 + side) * PLANE
            expand_packed(near, row, recv.at[slot, m, side, NEAR], reach)
            expand_packed(far, row, recv.at[slot, m, side, FAR], reach)
        deltas = [near[side_rows(m, side), :] for side in range(2)]
        faces = [middle[rows_of(m, i), :] + deltas[side] for side, i in enumerate(planes)]
        inside = inside_of(faces)
        for side, i in enumerate(planes):
            columns = slice(side * elements, (side + 1) * elements)
            value = (
                joint[side, 0] * faces[side]
                + joint[side, 1] * inside[:PLANE, columns]
                + joint[side, 2] * inside[PLANE:, columns]
                + cross[side] * deltas[1 - side]
                + beyond[side] * far[side_rows(m, side), :]
                + raw[side_rows(m, 1 - side), :]
            )
            store_lower(work, row_of(m, i), value)
            add_packed(work, row_of(m, i), recv.at[slot, m, side, NEXT])
        for i in planes:
            state[1 - slot, rows_of(m, i), :] = (
                state[0, rows_of(m, i), :] + final_reach * work[rows_of(m, i), :]
            )
        low, high = (final_reach * delta for delta in deltas)
        for i in range(1, ORDER):
            across = float(derivative[i, 0]) * low + float(derivative[i, ORDER]) * high
            store_assembled(work, row_of(m, i), speed[0, plane_rows(i), :] * across)
            state[1 - slot, rows_of(m, i), :] = ahead[rows_of(m, i), :] + work[rows_of(m, i), :]

    for m in range(members):
        take_masses(m)
        begin(m, 0)
        begin(m, ORDER)
        first_faces(0, m)
        first_inner(0, m)

    for copy in coef_copies():
        copy.wait()
    for side, i in enumerate((0, ORDER)):
        inverse = -time_step * work[rows_of(members, i), :]
        theirs = coef_recv[side, 0] * inverse
        ours = speed[0, plane_rows(i), :]
        joint[side, 0] = float(derivative[i, i]) * ours + (
            float(derivative[ORDER - i, ORDER - i]) * theirs
        )
        cross[side] = float(derivative[i, ORDER - i]) * ours
        beyond[side] = float(derivative[ORDER - i, i]) * theirs
        for r in (1, 2):
            joint[side, r] = speed[r, plane_rows(i), :] + coef_recv[side, r] * inverse
    for m in range(members):
        second_ahead(0, m)

    def stage(index, carry):
        for m in range(members):
            second(index - 1, m)
            first_faces(index, m)
            first_inner(index, m)
        for m in range(members):
            second_ahead(index, m)
        return carry

    final = 2 * SUBSTEPS - 1
    lax.fori_loop(1, final + 1, stage, 0)
    for m in range(members):
        second(final, m)


def slot_kernel(members, order, state, out):
    elements = order.shape[-1]
    lanes = lax.broadcasted_iota(jnp.int32, (elements, elements), 0)
    chosen = jnp.where(order[...] == lanes, 1.0, 0.0).astype(jnp.bfloat16)
    to_slot_matrix = jnp.concatenate([chosen, chosen], axis=0)
    for m in range(members):
        out[m, :, :] = jnp.dot(
            jnp.concatenate(halves(state[0, m * NODES : (m + 1) * NODES, :]), axis=1),
            to_slot_matrix,
            preferred_element_type=jnp.float32,
        )


def per_device(scalars, transport, mass, element_order):
    members, nodes, elements = scalars.shape
    count = lax.axis_size("elem")
    whole = pl.BlockSpec(memory_space=pltpu.VMEM)

    def floats(*shape):
        return pltpu.VMEM((*shape, elements), jnp.float32)

    def semaphores(*shape):
        return pltpu.SemaphoreType.DMA(shape)

    state = pl.pallas_call(
        functools.partial(kernel, count, members),
        out_shape=floats(2, members * nodes),
        in_specs=[whole] * 5,
        out_specs=whole,
        scratch_shapes=[
            floats(3, nodes),
            floats(members * nodes),
            floats(members * nodes),
            floats((members + 1) * nodes),
            floats(members * 2 * PLANE),
            floats(members * 2 * PLANE),
            floats(members * 2 * PLANE),
            floats(2, 3, PLANE),
            floats(2, PLANE),
            floats(2, PLANE),
            floats(members + 1, 2, PLANE - EXTENT),
            floats(members + 1, 2, PLANE - EXTENT),
            semaphores(members + 1, 2),
            semaphores(members + 1, 2),
            floats(2, 3, PLANE),
            floats(2, 3, PLANE),
            semaphores(2),
            semaphores(2),
            floats(2, members, 2, 2, PLANE - EXTENT),
            floats(2, members, 2, 3, PLANE - EXTENT),
            semaphores(2, members, 2, 3),
            semaphores(2, members, 2, 3),
        ],
        compiler_params=pltpu.CompilerParams(collective_id=0, has_side_effects=True),
    )(scalars, transport, mass, element_order, jnp.asarray(split_matrix()))
    return pl.pallas_call(
        functools.partial(slot_kernel, members),
        out_shape=jax.ShapeDtypeStruct(scalars.shape, jnp.float32),
        in_specs=[whole] * 2,
        out_specs=whole,
    )(element_order, pltpu.with_memory_space_constraint(state, pltpu.VMEM))


def solution(mesh):
    in_specs = (P("ens", None, "elem"), P(None, None, "elem"), P(None, "elem"), P("elem", None))
    out_specs = P("ens", None, "elem")
    return jax.shard_map(
        per_device, mesh=mesh, in_specs=in_specs, out_specs=out_specs, check_vma=False
    )
```

```python
import functools

import jax
import jax.numpy as jnp
import numpy as np
from jax import lax
from jax.experimental import pallas as pl
from jax.experimental.pallas import tpu as pltpu
from jax.sharding import PartitionSpec as P

ORDER = 7
SUBSTEPS = 2
EX = 1
EY = 8
EZ = 16
EXTENT = ORDER + 1
PLANE = EXTENT * EXTENT
NODES = EXTENT * PLANE
MESH = pl.DeviceIdType.MESH
NEAR, FAR, NEXT = 0, 1, 2


time_step = 0.015


def legendre_table(points, degree):
    table = np.zeros((points.shape[0], degree + 1))
    table[:, 0] = 1.0
    table[:, 1] = points
    for level in range(2, degree + 1):
        table[:, level] = (
            (2 * level - 1) * points * table[:, level - 1] - (level - 1) * table[:, level - 2]
        ) / level
    return table


def gll_derivative(degree):
    extent = degree + 1
    points = np.cos(np.pi * np.arange(extent) / degree)
    for sweep in range(60):
        table = legendre_table(points, degree)
        points = points - (points * table[:, degree] - table[:, degree - 1]) / (
            extent * table[:, degree]
        )
    points = points[::-1].copy()
    values = legendre_table(points, degree)[:, degree]
    matrix = np.zeros((extent, extent))
    for target in range(extent):
        for source in range(extent):
            if target != source:
                matrix[target, source] = values[target] / (
                    values[source] * (points[target] - points[source])
                )
    matrix[0, 0] = -degree * (degree + 1) / 4.0
    matrix[extent - 1, extent - 1] = degree * (degree + 1) / 4.0
    return matrix


def split_matrix():
    derivative = gll_derivative(ORDER).astype(np.float32)
    eye = np.eye(EXTENT, dtype=np.float32)
    full = np.concatenate([np.kron(derivative, eye), np.kron(eye, derivative)], axis=0)
    high = full.astype(jnp.bfloat16)
    low = (full - high.astype(np.float32)).astype(jnp.bfloat16)
    return np.concatenate([high, high, low], axis=1)


def halves(values):
    high = values.astype(jnp.bfloat16)
    low = (values - high.astype(jnp.float32)).astype(jnp.bfloat16)
    return high, low


def lane_forward(values, stride, length):
    total = values.shape[-1]
    near = pltpu.roll(values, total - stride, 1)
    if stride * length == total:
        return near
    coords = lax.broadcasted_iota(jnp.int32, values.shape, 1) // stride % length
    return jnp.where(coords < length - 1, near, pltpu.roll(values, stride * (length - 1), 1))


def lane_backward(values, stride, length):
    total = values.shape[-1]
    near = pltpu.roll(values, stride, 1)
    if stride * length == total:
        return near
    coords = lax.broadcasted_iota(jnp.int32, values.shape, 1) // stride % length
    return jnp.where(coords > 0, near, pltpu.roll(values, total - stride * (length - 1), 1))


def store_assembled(ref, row, values):
    low, high = values[:EXTENT], values[PLANE - EXTENT :]
    ref[row : row + EXTENT] = low + lane_backward(high, EZ, EY)
    ref[row + EXTENT : row + PLANE - EXTENT] = values[EXTENT : PLANE - EXTENT]
    ref[row + PLANE - EXTENT : row + PLANE] = high + lane_forward(low, EZ, EY)
    first = pl.ds(row, EXTENT, stride=EXTENT)
    last = pl.ds(row + ORDER, EXTENT, stride=EXTENT)
    k_low = ref[first, :]
    k_high = ref[last, :]
    ref[first, :] = k_low + lane_backward(k_high, 1, EZ)
    ref[last, :] = k_high + lane_forward(k_low, 1, EZ)


def store_lower(ref, row, values):
    low, high = values[:EXTENT], values[PLANE - EXTENT :]
    ref[row : row + EXTENT] = low + lane_backward(high, EZ, EY)
    ref[row + EXTENT : row + PLANE] = values[EXTENT:]
    first = pl.ds(row, EXTENT, stride=EXTENT)
    k_high = ref[pl.ds(row + ORDER, EXTENT, stride=EXTENT), :]
    ref[first, :] = ref[first, :] + lane_backward(k_high, 1, EZ)


def pack(source, row, target):
    for j in range(ORDER):
        target[j * ORDER : j * ORDER + EXTENT] = source[row + j * EXTENT : row + (j + 1) * EXTENT]


def add_packed(ref, row, packed):
    for j in range(ORDER):
        part = slice(row + j * EXTENT, row + (j + 1) * EXTENT)
        ref[part] = ref[part] + packed[j * ORDER : j * ORDER + EXTENT]
    k_low = ref[pl.ds(row, EXTENT, stride=EXTENT), :]
    ref[pl.ds(row + ORDER, EXTENT, stride=EXTENT), :] = lane_forward(k_low, 1, EZ)
    ref[row + PLANE - EXTENT : row + PLANE] = lane_forward(ref[row : row + EXTENT], EZ, EY)


def expand_packed(ref, row, packed, scale):
    for j in range(ORDER):
        ref[row + j * EXTENT : row + (j + 1) * EXTENT] = (
            scale * packed[j * ORDER : j * ORDER + EXTENT]
        )
    spread_lower(ref, row)


def spread_lower(ref, row):
    k_low = ref[pl.ds(row, EXTENT, stride=EXTENT), :]
    ref[pl.ds(row + ORDER, EXTENT, stride=EXTENT), :] = lane_forward(k_low, 1, EZ)
    ref[row + PLANE - EXTENT : row + PLANE] = lane_forward(ref[row : row + EXTENT], EZ, EY)


def kernel(
    count, members, groups, scalars_in, transport_in, mass_in, order_in, matrix_in, out,
    state,    scalars, transport, mass, order, matrix, load_sem, speed, middle, ahead, work, raw, near, far, joint, cross, beyond,
    mass_send, mass_recv, mass_send_sem, mass_recv_sem,
    coef_send, coef_recv, coef_send_sem, coef_recv_sem, share_send_sem, share_recv_sem,
    send, recv, send_sem, recv_sem,
):
    me, group = lax.axis_index("elem"), lax.axis_index("ens")

    def shifted(distance):
        return lax.rem(me + distance + count, count)

    def peer(distance):
        return {"ens": lax.rem(group + distance, groups)}

    barrier = pltpu.get_barrier_semaphore()
    for distance in (-2, -1, 1, 2):
        pl.semaphore_signal(
            barrier, inc=1, device_id={"elem": shifted(distance)}, device_id_type=MESH
        )
    for distance in range(1, groups):
        pl.semaphore_signal(barrier, inc=1, device_id=peer(distance), device_id_type=MESH)

    loads = [
        pltpu.make_async_copy(source, place, load_sem.at[number])
        for number, (source, place) in enumerate(
            (
                (order_in, order), (mass_in, mass), (scalars_in, scalars),
                (transport_in, transport), (matrix_in, matrix),
            )
        )
    ]
    for load in loads:
        load.start()
    loads[0].wait()

    elements = order.shape[-1]
    lanes = lax.broadcasted_iota(jnp.int32, (elements, elements), 0)
    chosen = jnp.where(order[...] == lanes, 1.0, 0.0).astype(jnp.bfloat16)
    to_brick_matrix = jnp.concatenate([chosen, chosen], axis=1)

    def to_brick(values):
        return lax.dot_general(
            jnp.concatenate(halves(values), axis=1),
            to_brick_matrix,
            (((1,), (1,)), ((), ())),
            preferred_element_type=jnp.float32,
        )

    first_side = 1 - lax.rem(me, 2)
    sides = (first_side, 1 - first_side)
    ends = (ORDER, 0)

    def target(side, distance):
        return {"elem": lax.rem(me + count + distance * (1 - 2 * side), count)}

    def mass_copies(m):
        return [
            pltpu.make_async_remote_copy(
                src_ref=mass_send.at[m, side, pl.ds(0, ORDER * ORDER)],
                dst_ref=mass_recv.at[m, side, pl.ds(0, ORDER * ORDER)],
                send_sem=mass_send_sem.at[m, side],
                recv_sem=mass_recv_sem.at[m, side],
                device_id=target(side, 1),
                device_id_type=MESH,
            )
            for side in sides
        ]

    share = 3 * PLANE // groups
    shared = pl.ds(pl.multiple_of(group * share, 8), share)

    def coef_copies():
        return [
            pltpu.make_async_remote_copy(
                src_ref=coef_send.at[side, shared],
                dst_ref=coef_recv.at[side, shared],
                send_sem=coef_send_sem.at[side],
                recv_sem=coef_recv_sem.at[side],
                device_id=target(side, 1),
                device_id_type=MESH,
            )
            for side in sides
        ]

    def share_copies():
        return [
            pltpu.make_async_remote_copy(
                src_ref=coef_recv.at[side, shared],
                dst_ref=coef_recv.at[side, shared],
                send_sem=share_send_sem.at[distance - 1, side],
                recv_sem=share_recv_sem.at[distance - 1, side],
                device_id=peer(distance),
                device_id_type=MESH,
            )
            for distance in range(1, groups)
            for side in sides
        ]

    def face_copies(slot, m, kinds):
        return [
            pltpu.make_async_remote_copy(
                src_ref=send.at[slot, m, side, kind // 2, pl.ds(0, ORDER * ORDER)],
                dst_ref=recv.at[slot, m, side, kind, pl.ds(0, ORDER * ORDER)],
                send_sem=send_sem.at[slot, m, side, kind],
                recv_sem=recv_sem.at[slot, m, side, kind],
                device_id=target(side, 2 if kind == FAR else 1),
                device_id_type=MESH,
            )
            for side in sides
            for kind in kinds
        ]

    def row_of(m, i):
        return (m * EXTENT + i) * PLANE

    def rows_of(m, i):
        return slice(row_of(m, i), row_of(m, i) + PLANE)

    def plane_rows(i):
        return slice(i * PLANE, (i + 1) * PLANE)

    def block(values, place):
        return values[place * PLANE : (place + 1) * PLANE]

    def side_rows(m, side):
        return slice((m * 2 + side) * PLANE, (m * 2 + side + 1) * PLANE)

    loads[1].wait()
    loads[2].wait()
    outer = to_brick(
        jnp.concatenate(
            [mass[plane_rows(i), :] for i in ends]
            + [scalars[m, plane_rows(i), :] for m in range(members) for i in ends],
            axis=0,
        )
    )
    for side, i in enumerate(ends):
        store_lower(work, row_of(members, i), block(outer, side))
        pack(work, row_of(members, i), mass_send.at[members, side])
    for m in range(members):
        for side, i in enumerate(ends):
            store_lower(
                work, row_of(m, i), block(outer, side) * block(outer, 2 * (m + 1) + side)
            )
            pack(work, row_of(m, i), mass_send.at[m, side])
    pl.semaphore_wait(barrier, 4 + groups - 1)
    for m in (members, *range(members)):
        for copy in mass_copies(m):
            copy.start()

    loads[3].wait()
    loads[4].wait()
    outer = to_brick(
        jnp.concatenate([transport[r, plane_rows(i), :] for r in range(3) for i in ends], axis=0)
    )
    for r in range(3):
        for side, i in enumerate(ends):
            speed[r, plane_rows(i), :] = block(outer, 2 * r + side)
            coef_send[side, plane_rows(r), :] = block(outer, 2 * r + side)
    for copy in coef_copies():
        copy.start()

    inner = slice(PLANE, NODES - PLANE)
    for r in range(3):
        speed[r, inner, :] = to_brick(transport[r, inner, :])
    middle[inner, :] = to_brick(mass[inner, :])
    for m in range(members):
        rows = slice(m * NODES + PLANE, (m + 1) * NODES - PLANE)
        ahead[rows, :] = to_brick(scalars[m, inner, :])
    for i in range(1, ORDER):
        weight = middle[plane_rows(i), :]
        store_assembled(work, row_of(members, i), weight)
        for m in range(members):
            store_assembled(work, row_of(m, i), weight * ahead[rows_of(m, i), :])

    def begin(m, i):
        state[0, rows_of(m, i), :] = work[rows_of(m, i), :] * work[rows_of(members, i), :]

    def scale(i):
        inverse = 1.0 / work[rows_of(members, i), :]
        work[rows_of(members, i), :] = inverse
        for r in range(3):
            speed[r, plane_rows(i), :] = speed[r, plane_rows(i), :] * (-time_step * inverse)

    for i in range(1, ORDER):
        scale(i)
        for m in range(members):
            begin(m, i)

    def take_masses(m):
        for copy in mass_copies(m):
            copy.wait()
        add_packed(work, row_of(m, 0), mass_recv.at[m, 0])
        add_packed(work, row_of(m, ORDER), mass_recv.at[m, 1])

    take_masses(members)
    scale(0)
    scale(ORDER)

    derivative = gll_derivative(ORDER)
    half = EXTENT // 2

    def inside_of(planes):
        stacked = []
        for values in planes:
            high, low = halves(values)
            stacked.append(jnp.concatenate([high, low, high], axis=0))
        return jnp.dot(
            matrix[...], jnp.concatenate(stacked, axis=1), preferred_element_type=jnp.float32
        )

    def pair(plane, a):
        even = odd = None
        for i in range(half):
            one, other = plane(i), plane(ORDER - i)
            plus = float(derivative[a, i] + derivative[a, ORDER - i]) * 0.5
            minus = float(derivative[a, i] - derivative[a, ORDER - i]) * 0.5
            even_term = plus * (one + other)
            odd_term = minus * (one - other)
            even = even_term if even is None else even + even_term
            odd = odd_term if odd is None else odd + odd_term
        inside = inside_of([plane(a), plane(ORDER - a)])
        for place, (i, across) in enumerate(((a, odd + even), (ORDER - a, odd - even))):
            columns = slice(place * elements, (place + 1) * elements)
            yield i, (
                speed[0, plane_rows(i), :] * across
                + speed[1, plane_rows(i), :] * inside[:PLANE, columns]
                + speed[2, plane_rows(i), :] * inside[PLANE:, columns]
            )

    def reaches(slot):
        return jnp.where(slot == 0, 0.25, 0.5), jnp.where(slot == 0, 1.0 / 3.0, 1.0)

    def first_faces(index, m):
        slot = lax.rem(index, 2)
        for i, value in pair(lambda n: state[slot, rows_of(m, n), :], 0):
            side = ends.index(i)
            store_lower(work, row_of(m, i), value)
            pack(work, row_of(m, i), send.at[slot, m, side, 0])
        for copy in face_copies(slot, m, (FAR, NEAR)):
            copy.start()

    def first_inner(index, m):
        slot = lax.rem(index, 2)
        reach, _ = reaches(slot)
        for i in ends:
            spread_lower(work, row_of(m, i))
            middle[rows_of(m, i), :] = state[0, rows_of(m, i), :] + reach * work[rows_of(m, i), :]
        for a in range(1, half):
            for i, value in pair(lambda n: state[slot, rows_of(m, n), :], a):
                store_assembled(work, row_of(m, i), value)
                middle[rows_of(m, i), :] = (
                    state[0, rows_of(m, i), :] + reach * work[rows_of(m, i), :]
                )
        for side, i in enumerate(ends):
            across = None
            for n in range(EXTENT):
                if n != i:
                    term = float(derivative[i, n]) * middle[rows_of(m, n), :]
                    across = term if across is None else across + term
            value = speed[0, plane_rows(i), :] * across
            raw[side_rows(m, side), :] = value
            store_lower(work, row_of(m, i), value)
            pack(work, row_of(m, i), send.at[slot, m, side, 1])
        for copy in face_copies(slot, m, (NEXT,)):
            copy.start()

    def second_ahead(index, m):
        _, reach = reaches(lax.rem(index, 2))
        for a in range(1, half):
            for i, value in pair(lambda n: middle[rows_of(m, n), :], a):
                store_assembled(work, row_of(m, i), value)
                ahead[rows_of(m, i), :] = (
                    state[0, rows_of(m, i), :] + reach * work[rows_of(m, i), :]
                )

    def second(index, m):
        slot = lax.rem(index, 2)
        reach, final_reach = reaches(slot)
        for copy in face_copies(slot, m, (NEAR, FAR, NEXT)):
            copy.wait()
        planes = (0, ORDER)
        for side, i in enumerate(planes):
            row = (m * 2 + side) * PLANE
            expand_packed(near, row, recv.at[slot, m, side, NEAR], reach)
            expand_packed(far, row, recv.at[slot, m, side, FAR], reach)
        deltas = [near[side_rows(m, side), :] for side in range(2)]
        faces = [middle[rows_of(m, i), :] + deltas[side] for side, i in enumerate(planes)]
        inside = inside_of(faces)
        for side, i in enumerate(planes):
            columns = slice(side * elements, (side + 1) * elements)
            value = (
                joint[side, 0] * faces[side]
                + joint[side, 1] * inside[:PLANE, columns]
                + joint[side, 2] * inside[PLANE:, columns]
                + cross[side] * deltas[1 - side]
                + beyond[side] * far[side_rows(m, side), :]
                + raw[side_rows(m, 1 - side), :]
            )
            store_lower(work, row_of(m, i), value)
            add_packed(work, row_of(m, i), recv.at[slot, m, side, NEXT])
        for i in planes:
            state[1 - slot, rows_of(m, i), :] = (
                state[0, rows_of(m, i), :] + final_reach * work[rows_of(m, i), :]
            )
        low, high = (final_reach * delta for delta in deltas)
        for i in range(1, ORDER):
            across = float(derivative[i, 0]) * low + float(derivative[i, ORDER]) * high
            store_assembled(work, row_of(m, i), speed[0, plane_rows(i), :] * across)
            state[1 - slot, rows_of(m, i), :] = ahead[rows_of(m, i), :] + work[rows_of(m, i), :]

    for m in range(members):
        take_masses(m)
        begin(m, 0)
        begin(m, ORDER)
        first_faces(0, m)
        first_inner(0, m)

    for copy in coef_copies():
        copy.wait()
    for copy in share_copies():
        copy.start()
    for copy in share_copies():
        copy.wait()
    for side, i in enumerate((0, ORDER)):
        inverse = -time_step * work[rows_of(members, i), :]
        theirs = coef_recv[side, plane_rows(0), :] * inverse
        ours = speed[0, plane_rows(i), :]
        joint[side, 0] = float(derivative[i, i]) * ours + (
            float(derivative[ORDER - i, ORDER - i]) * theirs
        )
        cross[side] = float(derivative[i, ORDER - i]) * ours
        beyond[side] = float(derivative[ORDER - i, i]) * theirs
        for r in (1, 2):
            joint[side, r] = speed[r, plane_rows(i), :] + coef_recv[side, plane_rows(r), :] * inverse
    for m in range(members):
        second_ahead(0, m)

    def stage(index, carry):
        for m in range(members):
            second(index - 1, m)
            first_faces(index, m)
            first_inner(index, m)
        for m in range(members):
            second_ahead(index, m)
        return carry

    final = 2 * SUBSTEPS - 1
    lax.fori_loop(1, final + 1, stage, 0)
    for m in range(members):
        second(final, m)
        out[m, :, :] = jnp.dot(
            jnp.concatenate(halves(state[0, m * NODES : (m + 1) * NODES, :]), axis=1),
            jnp.concatenate([chosen, chosen], axis=0),
            preferred_element_type=jnp.float32,
        )


def store_kernel(result, out, store_sem):
    copy = pltpu.make_async_copy(result, out, store_sem)
    copy.start()
    copy.wait()


def per_device(scalars, transport, mass, element_order):
    members, nodes, elements = scalars.shape
    count, groups = lax.axis_size("elem"), lax.axis_size("ens")
    whole = pl.BlockSpec(memory_space=pltpu.VMEM)
    matrix = jnp.asarray(split_matrix())

    def floats(*shape):
        return pltpu.VMEM((*shape, elements), jnp.float32)

    def semaphores(*shape):
        return pltpu.SemaphoreType.DMA(shape)

    result = pl.pallas_call(
        functools.partial(kernel, count, members, groups),
        out_shape=floats(members, nodes),
        in_specs=[pl.BlockSpec(memory_space=pl.ANY)] * 5,
        out_specs=whole,
        scratch_shapes=[
            floats(2, members * nodes),
            floats(members, nodes),
            floats(3, nodes),
            floats(nodes),
            pltpu.VMEM(element_order.shape, jnp.int32),
            pltpu.VMEM(matrix.shape, matrix.dtype),
            semaphores(5),
            floats(3, nodes),
            floats(members * nodes),
            floats(members * nodes),
            floats((members + 1) * nodes),
            floats(members * 2 * PLANE),
            floats(members * 2 * PLANE),
            floats(members * 2 * PLANE),
            floats(2, 3, PLANE),
            floats(2, PLANE),
            floats(2, PLANE),
            floats(members + 1, 2, PLANE - EXTENT),
            floats(members + 1, 2, PLANE - EXTENT),
            semaphores(members + 1, 2),
            semaphores(members + 1, 2),
            floats(2, 3 * PLANE),
            floats(2, 3 * PLANE),
            semaphores(2),
            semaphores(2),
            semaphores(groups - 1, 2),
            semaphores(groups - 1, 2),
            floats(2, members, 2, 2, PLANE - EXTENT),
            floats(2, members, 2, 3, PLANE - EXTENT),
            semaphores(2, members, 2, 3),
            semaphores(2, members, 2, 3),
        ],
        compiler_params=pltpu.CompilerParams(collective_id=0, has_side_effects=True),
    )(scalars, transport, mass, element_order, matrix)
    return pl.pallas_call(
        store_kernel,
        out_shape=jax.ShapeDtypeStruct(scalars.shape, jnp.float32),
        in_specs=[whole],
        out_specs=pl.BlockSpec(memory_space=pl.ANY),
        scratch_shapes=[pltpu.SemaphoreType.DMA],
    )(pltpu.with_memory_space_constraint(result, pltpu.VMEM))


def solution(mesh):
    in_specs = (P("ens", None, "elem"), P(None, None, "elem"), P(None, "elem"), P("elem", None))
    out_specs = P("ens", None, "elem")
    return jax.shard_map(
        per_device, mesh=mesh, in_specs=in_specs, out_specs=out_specs, check_vma=False
    )
```

```python
import functools

import jax
import jax.numpy as jnp
import numpy as np
from jax import lax
from jax.experimental import pallas as pl
from jax.experimental.pallas import tpu as pltpu
from jax.sharding import PartitionSpec as P

ORDER = 7
SUBSTEPS = 2
EX = 1
EY = 8
EZ = 16
EXTENT = ORDER + 1
PLANE = EXTENT * EXTENT
NODES = EXTENT * PLANE
MESH = pl.DeviceIdType.MESH
NEAR, FAR, NEXT = 0, 1, 2


time_step = 0.015


def legendre_table(points, degree):
    table = np.zeros((points.shape[0], degree + 1))
    table[:, 0] = 1.0
    table[:, 1] = points
    for level in range(2, degree + 1):
        table[:, level] = (
            (2 * level - 1) * points * table[:, level - 1] - (level - 1) * table[:, level - 2]
        ) / level
    return table


def gll_derivative(degree):
    extent = degree + 1
    points = np.cos(np.pi * np.arange(extent) / degree)
    for sweep in range(60):
        table = legendre_table(points, degree)
        points = points - (points * table[:, degree] - table[:, degree - 1]) / (
            extent * table[:, degree]
        )
    points = points[::-1].copy()
    values = legendre_table(points, degree)[:, degree]
    matrix = np.zeros((extent, extent))
    for target in range(extent):
        for source in range(extent):
            if target != source:
                matrix[target, source] = values[target] / (
                    values[source] * (points[target] - points[source])
                )
    matrix[0, 0] = -degree * (degree + 1) / 4.0
    matrix[extent - 1, extent - 1] = degree * (degree + 1) / 4.0
    return matrix


def split_matrix():
    derivative = gll_derivative(ORDER).astype(np.float32)
    eye = np.eye(EXTENT, dtype=np.float32)
    full = np.concatenate([np.kron(derivative, eye), np.kron(eye, derivative)], axis=0)
    high = full.astype(jnp.bfloat16)
    low = (full - high.astype(np.float32)).astype(jnp.bfloat16)
    return np.concatenate([high, high, low], axis=1)


def halves(values):
    high = values.astype(jnp.bfloat16)
    low = (values - high.astype(jnp.float32)).astype(jnp.bfloat16)
    return high, low


def lane_forward(values, stride, length):
    total = values.shape[-1]
    near = pltpu.roll(values, total - stride, 1)
    if stride * length == total:
        return near
    coords = lax.broadcasted_iota(jnp.int32, values.shape, 1) // stride % length
    return jnp.where(coords < length - 1, near, pltpu.roll(values, stride * (length - 1), 1))


def lane_backward(values, stride, length):
    total = values.shape[-1]
    near = pltpu.roll(values, stride, 1)
    if stride * length == total:
        return near
    coords = lax.broadcasted_iota(jnp.int32, values.shape, 1) // stride % length
    return jnp.where(coords > 0, near, pltpu.roll(values, total - stride * (length - 1), 1))


def store_assembled(ref, row, values):
    low, high = values[:EXTENT], values[PLANE - EXTENT :]
    ref[row : row + EXTENT] = low + lane_backward(high, EZ, EY)
    ref[row + EXTENT : row + PLANE - EXTENT] = values[EXTENT : PLANE - EXTENT]
    ref[row + PLANE - EXTENT : row + PLANE] = high + lane_forward(low, EZ, EY)
    first = pl.ds(row, EXTENT, stride=EXTENT)
    last = pl.ds(row + ORDER, EXTENT, stride=EXTENT)
    k_low = ref[first, :]
    k_high = ref[last, :]
    ref[first, :] = k_low + lane_backward(k_high, 1, EZ)
    ref[last, :] = k_high + lane_forward(k_low, 1, EZ)


LOWER = PLANE - EXTENT
SENT = ORDER * ORDER
TAIL = LOWER - EXTENT


def lines_of(values, count):
    return [values[j * EXTENT : (j + 1) * EXTENT] for j in range(count)]


def sublanes_of(line):
    return lax.broadcasted_iota(jnp.int32, line.shape, 0)


def gather_points(lines, k):
    rows = sublanes_of(lines[0])
    points = pltpu.roll(lines[0], (EXTENT - k) % EXTENT, 0) if k else lines[0]
    for j, line in enumerate(lines):
        if j:
            moved = pltpu.roll(line, (j - k) % EXTENT, 0) if (j - k) % EXTENT else line
            points = jnp.where(rows == j, moved, points)
    return points


def point_at(points, j, k):
    return pltpu.roll(points, (k - j) % EXTENT, 0) if (k - j) % EXTENT else points


def lower_of(values):
    lines = lines_of(values, EXTENT)
    lines = [lines[0] + lane_backward(lines[ORDER], EZ, EY)] + lines[1:ORDER]
    back = lane_backward(gather_points(lines, ORDER), 1, EZ)
    rows = sublanes_of(back)
    return [
        jnp.where(rows == 0, line + point_at(back, j, 0), line) for j, line in enumerate(lines)
    ]


def assembled_of(values):
    lines = lines_of(values, EXTENT)
    low = lines[0] + lane_backward(lines[ORDER], EZ, EY)
    high = lines[ORDER] + lane_forward(lines[0], EZ, EY)
    lines = [low] + lines[1:ORDER] + [high]
    back = lane_backward(gather_points(lines, ORDER), 1, EZ)
    ahead = lane_forward(gather_points(lines, 0), 1, EZ)
    rows = sublanes_of(back)
    return [
        jnp.where(
            rows == 0,
            line + point_at(back, j, 0),
            jnp.where(rows == ORDER, line + point_at(ahead, j, ORDER), line),
        )
        for j, line in enumerate(lines)
    ]


def spread_of(lines):
    ahead = lane_forward(gather_points(lines, 0), 1, EZ)
    rows = sublanes_of(ahead)
    lines = [
        jnp.where(rows == ORDER, point_at(ahead, j, ORDER), line) for j, line in enumerate(lines)
    ]
    return lines + [lane_forward(lines[0], EZ, EY)]


def plane_of(lines):
    return jnp.concatenate(lines, axis=0)


def store_sent(ref, lines):
    tail = lines[ORDER - 1]
    rows = sublanes_of(tail)
    for j in range(ORDER - 1):
        ref[j * EXTENT : (j + 1) * EXTENT] = jnp.where(
            rows == ORDER, point_at(tail, j + 1, ORDER), lines[j]
        )
    ref[TAIL:LOWER] = tail


def received(packed):
    tail = packed[pl.ds(ORDER, EXTENT, stride=EXTENT), :]
    rows = sublanes_of(tail)
    tail = jnp.where(rows == 0, packed[LOWER : LOWER + EXTENT], tail)
    return lines_of(packed[EXTENT:LOWER], ORDER - 1) + [tail]


def add_lines(one, other):
    return [a + b for a, b in zip(one, other)]


def kernel(
    count, members, groups, scalars_in, transport_in, mass_in, order_in, matrix_in, out,
    state,    scalars, transport, mass, order, matrix, load_sem, speed, middle, ahead, work, raw, joint, cross, beyond,
    mass_send, mass_recv, mass_send_sem, mass_recv_sem,
    coef_send, coef_recv, coef_send_sem, coef_recv_sem, share_send_sem, share_recv_sem,
    send, recv, send_sem, recv_sem,
):
    me, group = lax.axis_index("elem"), lax.axis_index("ens")

    def shifted(distance):
        return lax.rem(me + distance + count, count)

    def peer(distance):
        return {"ens": lax.rem(group + distance, groups)}

    barrier = pltpu.get_barrier_semaphore()
    for distance in (-2, -1, 1, 2):
        pl.semaphore_signal(
            barrier, inc=1, device_id={"elem": shifted(distance)}, device_id_type=MESH
        )
    for distance in range(1, groups):
        pl.semaphore_signal(barrier, inc=1, device_id=peer(distance), device_id_type=MESH)

    loads = [
        pltpu.make_async_copy(source, place, load_sem.at[number])
        for number, (source, place) in enumerate(
            (
                (order_in, order), (mass_in, mass), (scalars_in, scalars),
                (transport_in, transport), (matrix_in, matrix),
            )
        )
    ]
    for load in loads:
        load.start()
    loads[0].wait()

    elements = order.shape[-1]
    lanes = lax.broadcasted_iota(jnp.int32, (elements, elements), 0)
    chosen = jnp.where(order[...] == lanes, 1.0, 0.0).astype(jnp.bfloat16)
    to_brick_matrix = jnp.concatenate([chosen, chosen], axis=1)

    def to_brick(values):
        return lax.dot_general(
            jnp.concatenate(halves(values), axis=1),
            to_brick_matrix,
            (((1,), (1,)), ((), ())),
            preferred_element_type=jnp.float32,
        )

    first_side = 1 - lax.rem(me, 2)
    sides = (first_side, 1 - first_side)
    ends = (ORDER, 0)

    def target(side, distance):
        return {"elem": lax.rem(me + count + distance * (1 - 2 * side), count)}

    def mass_copies(m):
        return [
            pltpu.make_async_remote_copy(
                src_ref=mass_send.at[m, side, pl.ds(0, SENT)],
                dst_ref=mass_recv.at[m, side, pl.ds(EXTENT, SENT)],
                send_sem=mass_send_sem.at[m, side],
                recv_sem=mass_recv_sem.at[m, side],
                device_id=target(side, 1),
                device_id_type=MESH,
            )
            for side in sides
        ]

    share = 3 * PLANE // groups
    shared = pl.ds(pl.multiple_of(group * share, 8), share)

    def coef_copies():
        return [
            pltpu.make_async_remote_copy(
                src_ref=coef_send.at[side, shared],
                dst_ref=coef_recv.at[side, shared],
                send_sem=coef_send_sem.at[side],
                recv_sem=coef_recv_sem.at[side],
                device_id=target(side, 1),
                device_id_type=MESH,
            )
            for side in sides
        ]

    def share_copies():
        return [
            pltpu.make_async_remote_copy(
                src_ref=coef_recv.at[side, shared],
                dst_ref=coef_recv.at[side, shared],
                send_sem=share_send_sem.at[distance - 1, side],
                recv_sem=share_recv_sem.at[distance - 1, side],
                device_id=peer(distance),
                device_id_type=MESH,
            )
            for distance in range(1, groups)
            for side in sides
        ]

    def face_copies(slot, m, kinds):
        return [
            pltpu.make_async_remote_copy(
                src_ref=send.at[slot, m, side, kind // 2, pl.ds(0, SENT)],
                dst_ref=recv.at[slot, m, side, kind, pl.ds(EXTENT, SENT)],
                send_sem=send_sem.at[slot, m, side, kind],
                recv_sem=recv_sem.at[slot, m, side, kind],
                device_id=target(side, 2 if kind == FAR else 1),
                device_id_type=MESH,
            )
            for side in sides
            for kind in kinds
        ]

    def row_of(m, i):
        return (m * EXTENT + i) * PLANE

    def rows_of(m, i):
        return slice(row_of(m, i), row_of(m, i) + PLANE)

    def lower_rows(m, i):
        return slice(row_of(m, i), row_of(m, i) + LOWER)

    def plane_rows(i):
        return slice(i * PLANE, (i + 1) * PLANE)

    def block(values, place):
        return values[place * PLANE : (place + 1) * PLANE]

    def side_rows(m, side):
        return slice((m * 2 + side) * PLANE, (m * 2 + side + 1) * PLANE)

    loads[1].wait()
    loads[2].wait()
    outer = to_brick(
        jnp.concatenate(
            [mass[plane_rows(i), :] for i in ends]
            + [scalars[m, plane_rows(i), :] for m in range(members) for i in ends],
            axis=0,
        )
    )
    for side, i in enumerate(ends):
        lines = lower_of(block(outer, side))
        work[lower_rows(members, i), :] = plane_of(lines)
        store_sent(mass_send.at[members, side], lines)
    for m in range(members):
        for side, i in enumerate(ends):
            lines = lower_of(block(outer, side) * block(outer, 2 * (m + 1) + side))
            work[lower_rows(m, i), :] = plane_of(lines)
            store_sent(mass_send.at[m, side], lines)
    loads[3].wait()
    loads[4].wait()
    outer = to_brick(
        jnp.concatenate([transport[r, plane_rows(i), :] for r in range(3) for i in ends], axis=0)
    )
    for r in range(3):
        for side, i in enumerate(ends):
            speed[r, plane_rows(i), :] = block(outer, 2 * r + side)
            coef_send[side, plane_rows(r), :] = block(outer, 2 * r + side)
    pl.semaphore_wait(barrier, 4 + groups - 1)
    for m in (members, *range(members)):
        for copy in mass_copies(m):
            copy.start()

    for copy in coef_copies():
        copy.start()

    inner = slice(PLANE, NODES - PLANE)
    for r in range(3):
        speed[r, inner, :] = to_brick(transport[r, inner, :])
    middle[inner, :] = to_brick(mass[inner, :])
    for m in range(members):
        rows = slice(m * NODES + PLANE, (m + 1) * NODES - PLANE)
        ahead[rows, :] = to_brick(scalars[m, inner, :])
    for i in range(1, ORDER):
        weight = middle[plane_rows(i), :]
        store_assembled(work, row_of(members, i), weight)
        for m in range(members):
            store_assembled(work, row_of(m, i), weight * ahead[rows_of(m, i), :])

    def begin(m, i):
        state[0, rows_of(m, i), :] = work[rows_of(m, i), :] * work[rows_of(members, i), :]

    def scale(i):
        inverse = 1.0 / work[rows_of(members, i), :]
        work[rows_of(members, i), :] = inverse
        for r in range(3):
            speed[r, plane_rows(i), :] = speed[r, plane_rows(i), :] * (-time_step * inverse)

    for i in range(1, ORDER):
        scale(i)
        for m in range(members):
            begin(m, i)

    def take_masses(m):
        for copy in mass_copies(m):
            copy.wait()
        for side, i in enumerate((0, ORDER)):
            own = lines_of(work[lower_rows(m, i), :], ORDER)
            lines = add_lines(own, received(mass_recv.at[m, side]))
            work[rows_of(m, i), :] = plane_of(spread_of(lines))

    take_masses(members)
    scale(0)
    scale(ORDER)

    derivative = gll_derivative(ORDER)
    half = EXTENT // 2

    def inside_of(planes):
        stacked = []
        for values in planes:
            high, low = halves(values)
            stacked.append(jnp.concatenate([high, low, high], axis=0))
        return jnp.dot(
            matrix[...], jnp.concatenate(stacked, axis=1), preferred_element_type=jnp.float32
        )

    def pair(plane, a):
        even = odd = None
        for i in range(half):
            one, other = plane(i), plane(ORDER - i)
            plus = float(derivative[a, i] + derivative[a, ORDER - i]) * 0.5
            minus = float(derivative[a, i] - derivative[a, ORDER - i]) * 0.5
            even_term = plus * (one + other)
            odd_term = minus * (one - other)
            even = even_term if even is None else even + even_term
            odd = odd_term if odd is None else odd + odd_term
        inside = inside_of([plane(a), plane(ORDER - a)])
        for place, (i, across) in enumerate(((a, odd + even), (ORDER - a, odd - even))):
            columns = slice(place * elements, (place + 1) * elements)
            yield i, (
                speed[0, plane_rows(i), :] * across
                + speed[1, plane_rows(i), :] * inside[:PLANE, columns]
                + speed[2, plane_rows(i), :] * inside[PLANE:, columns]
            )

    def reaches(slot):
        return jnp.where(slot == 0, 0.25, 0.5), jnp.where(slot == 0, 1.0 / 3.0, 1.0)

    def first_faces(index, m):
        slot = lax.rem(index, 2)
        for i, value in pair(lambda n: state[slot, rows_of(m, n), :], 0):
            lines = lower_of(value)
            store_sent(send.at[slot, m, ends.index(i), 0], lines)
            work[rows_of(m, i), :] = plane_of(spread_of(lines))
        for copy in face_copies(slot, m, (NEAR,)):
            copy.start()

    def first_inner(index, m):
        slot = lax.rem(index, 2)
        reach, _ = reaches(slot)
        for i in ends:
            middle[rows_of(m, i), :] = state[0, rows_of(m, i), :] + reach * work[rows_of(m, i), :]
        for a in range(1, half):
            for i, value in pair(lambda n: state[slot, rows_of(m, n), :], a):
                store_assembled(work, row_of(m, i), value)
                middle[rows_of(m, i), :] = (
                    state[0, rows_of(m, i), :] + reach * work[rows_of(m, i), :]
                )
        for side, i in enumerate(ends):
            across = None
            for n in range(EXTENT):
                if n != i:
                    term = float(derivative[i, n]) * middle[rows_of(m, n), :]
                    across = term if across is None else across + term
            value = speed[0, plane_rows(i), :] * across
            raw[side_rows(m, side), :] = value
            store_sent(send.at[slot, m, side, 1], lower_of(value))
        for copy in face_copies(slot, m, (NEXT, FAR)):
            copy.start()

    def second_ahead(index, m):
        _, reach = reaches(lax.rem(index, 2))
        for a in range(1, half):
            for i, value in pair(lambda n: middle[rows_of(m, n), :], a):
                store_assembled(work, row_of(m, i), value)
                ahead[rows_of(m, i), :] = (
                    state[0, rows_of(m, i), :] + reach * work[rows_of(m, i), :]
                )

    def second(index, m):
        slot = lax.rem(index, 2)
        reach, final_reach = reaches(slot)
        for copy in face_copies(slot, m, (NEAR, FAR, NEXT)):
            copy.wait()
        planes = (0, ORDER)

        def taken(side, kind):
            return spread_of(received(recv.at[slot, m, side, kind]))

        deltas = [reach * plane_of(taken(side, NEAR)) for side in range(2)]
        faces = [middle[rows_of(m, i), :] + deltas[side] for side, i in enumerate(planes)]
        inside = inside_of(faces)
        for side, i in enumerate(planes):
            columns = slice(side * elements, (side + 1) * elements)
            value = (
                joint[side, 0] * faces[side]
                + joint[side, 1] * inside[:PLANE, columns]
                + joint[side, 2] * inside[PLANE:, columns]
                + cross[side] * deltas[1 - side]
                + beyond[side] * (reach * plane_of(taken(side, FAR)))
                + raw[side_rows(m, 1 - side), :]
            )
            total = add_lines(assembled_of(value), taken(side, NEXT))
            state[1 - slot, rows_of(m, i), :] = (
                state[0, rows_of(m, i), :] + final_reach * plane_of(total)
            )
        low, high = (final_reach * delta for delta in deltas)
        for i in range(1, ORDER):
            across = float(derivative[i, 0]) * low + float(derivative[i, ORDER]) * high
            store_assembled(work, row_of(m, i), speed[0, plane_rows(i), :] * across)
            state[1 - slot, rows_of(m, i), :] = ahead[rows_of(m, i), :] + work[rows_of(m, i), :]

    for m in range(members):
        take_masses(m)
        begin(m, 0)
        begin(m, ORDER)
        first_faces(0, m)
        first_inner(0, m)
        if m == 0:
            for copy in coef_copies():
                copy.wait()
            for copy in share_copies():
                copy.start()

    for m in range(members):
        second_ahead(0, m)
    for copy in share_copies():
        copy.wait()
    for side, i in enumerate((0, ORDER)):
        inverse = -time_step * work[rows_of(members, i), :]
        theirs = coef_recv[side, plane_rows(0), :] * inverse
        ours = speed[0, plane_rows(i), :]
        joint[side, 0] = float(derivative[i, i]) * ours + (
            float(derivative[ORDER - i, ORDER - i]) * theirs
        )
        cross[side] = float(derivative[i, ORDER - i]) * ours
        beyond[side] = float(derivative[ORDER - i, i]) * theirs
        for r in (1, 2):
            joint[side, r] = speed[r, plane_rows(i), :] + coef_recv[side, plane_rows(r), :] * inverse

    def stage(index, carry):
        for m in range(members):
            second(index - 1, m)
            first_faces(index, m)
            first_inner(index, m)
        for m in range(members):
            second_ahead(index, m)
        return carry

    final = 2 * SUBSTEPS - 1
    lax.fori_loop(1, final + 1, stage, 0)
    for m in range(members):
        second(final, m)
        out[m, :, :] = jnp.dot(
            jnp.concatenate(halves(state[0, m * NODES : (m + 1) * NODES, :]), axis=1),
            jnp.concatenate([chosen, chosen], axis=0),
            preferred_element_type=jnp.float32,
        )


def store_kernel(result, out, store_sem):
    copy = pltpu.make_async_copy(result, out, store_sem)
    copy.start()
    copy.wait()


def per_device(scalars, transport, mass, element_order):
    members, nodes, elements = scalars.shape
    count, groups = lax.axis_size("elem"), lax.axis_size("ens")
    whole = pl.BlockSpec(memory_space=pltpu.VMEM)
    matrix = jnp.asarray(split_matrix())

    def floats(*shape):
        return pltpu.VMEM((*shape, elements), jnp.float32)

    def semaphores(*shape):
        return pltpu.SemaphoreType.DMA(shape)

    result = pl.pallas_call(
        functools.partial(kernel, count, members, groups),
        out_shape=floats(members, nodes),
        in_specs=[pl.BlockSpec(memory_space=pl.ANY)] * 5,
        out_specs=whole,
        scratch_shapes=[
            floats(2, members * nodes),
            floats(members, nodes),
            floats(3, nodes),
            floats(nodes),
            pltpu.VMEM(element_order.shape, jnp.int32),
            pltpu.VMEM(matrix.shape, matrix.dtype),
            semaphores(5),
            floats(3, nodes),
            floats(members * nodes),
            floats(members * nodes),
            floats((members + 1) * nodes),
            floats(members * 2 * PLANE),
            floats(2, 3, PLANE),
            floats(2, PLANE),
            floats(2, PLANE),
            floats(members + 1, 2, PLANE),
            floats(members + 1, 2, PLANE),
            semaphores(members + 1, 2),
            semaphores(members + 1, 2),
            floats(2, 3 * PLANE),
            floats(2, 3 * PLANE),
            semaphores(2),
            semaphores(2),
            semaphores(groups - 1, 2),
            semaphores(groups - 1, 2),
            floats(2, members, 2, 2, PLANE),
            floats(2, members, 2, 3, PLANE),
            semaphores(2, members, 2, 3),
            semaphores(2, members, 2, 3),
        ],
        compiler_params=pltpu.CompilerParams(collective_id=0, has_side_effects=True),
    )(scalars, transport, mass, element_order, matrix)
    return pl.pallas_call(
        store_kernel,
        out_shape=jax.ShapeDtypeStruct(scalars.shape, jnp.float32),
        in_specs=[whole],
        out_specs=pl.BlockSpec(memory_space=pl.ANY),
        scratch_shapes=[pltpu.SemaphoreType.DMA],
    )(pltpu.with_memory_space_constraint(result, pltpu.VMEM))


def solution(mesh):
    in_specs = (P("ens", None, "elem"), P(None, None, "elem"), P(None, "elem"), P("elem", None))
    out_specs = P("ens", None, "elem")
    return jax.shard_map(
        per_device, mesh=mesh, in_specs=in_specs, out_specs=out_specs, check_vma=False
    )
```

```python
import functools

import jax
import jax.numpy as jnp
import numpy as np
from jax import lax
from jax.experimental import pallas as pl
from jax.experimental.pallas import tpu as pltpu
from jax.sharding import PartitionSpec as P

ORDER = 7
SUBSTEPS = 2
EX = 1
EY = 8
EZ = 16
EXTENT = ORDER + 1
PLANE = EXTENT * EXTENT
NODES = EXTENT * PLANE
MESH = pl.DeviceIdType.MESH
NEAR, FAR, NEXT = 0, 1, 2


time_step = 0.015


def legendre_table(points, degree):
    table = np.zeros((points.shape[0], degree + 1))
    table[:, 0] = 1.0
    table[:, 1] = points
    for level in range(2, degree + 1):
        table[:, level] = (
            (2 * level - 1) * points * table[:, level - 1] - (level - 1) * table[:, level - 2]
        ) / level
    return table


def gll_derivative(degree):
    extent = degree + 1
    points = np.cos(np.pi * np.arange(extent) / degree)
    for sweep in range(60):
        table = legendre_table(points, degree)
        points = points - (points * table[:, degree] - table[:, degree - 1]) / (
            extent * table[:, degree]
        )
    points = points[::-1].copy()
    values = legendre_table(points, degree)[:, degree]
    matrix = np.zeros((extent, extent))
    for target in range(extent):
        for source in range(extent):
            if target != source:
                matrix[target, source] = values[target] / (
                    values[source] * (points[target] - points[source])
                )
    matrix[0, 0] = -degree * (degree + 1) / 4.0
    matrix[extent - 1, extent - 1] = degree * (degree + 1) / 4.0
    return matrix


def split_matrix():
    derivative = gll_derivative(ORDER).astype(np.float32)
    eye = np.eye(EXTENT, dtype=np.float32)
    full = np.concatenate([np.kron(derivative, eye), np.kron(eye, derivative)], axis=0)
    high = full.astype(jnp.bfloat16)
    low = (full - high.astype(np.float32)).astype(jnp.bfloat16)
    return np.concatenate([high, high, low], axis=1)


def halves(values):
    high = values.astype(jnp.bfloat16)
    low = (values - high.astype(jnp.float32)).astype(jnp.bfloat16)
    return high, low


def lane_forward(values, stride, length):
    total = values.shape[-1]
    near = pltpu.roll(values, total - stride, 1)
    if stride * length == total:
        return near
    coords = lax.broadcasted_iota(jnp.int32, values.shape, 1) // stride % length
    return jnp.where(coords < length - 1, near, pltpu.roll(values, stride * (length - 1), 1))


def lane_backward(values, stride, length):
    total = values.shape[-1]
    near = pltpu.roll(values, stride, 1)
    if stride * length == total:
        return near
    coords = lax.broadcasted_iota(jnp.int32, values.shape, 1) // stride % length
    return jnp.where(coords > 0, near, pltpu.roll(values, total - stride * (length - 1), 1))


def store_assembled(ref, row, values):
    low, high = values[:EXTENT], values[PLANE - EXTENT :]
    ref[row : row + EXTENT] = low + lane_backward(high, EZ, EY)
    ref[row + EXTENT : row + PLANE - EXTENT] = values[EXTENT : PLANE - EXTENT]
    ref[row + PLANE - EXTENT : row + PLANE] = high + lane_forward(low, EZ, EY)
    first = pl.ds(row, EXTENT, stride=EXTENT)
    last = pl.ds(row + ORDER, EXTENT, stride=EXTENT)
    k_low = ref[first, :]
    k_high = ref[last, :]
    ref[first, :] = k_low + lane_backward(k_high, 1, EZ)
    ref[last, :] = k_high + lane_forward(k_low, 1, EZ)


LOWER = PLANE - EXTENT
SENT = ORDER * ORDER
TAIL = LOWER - EXTENT


def lines_of(values, count):
    return [values[j * EXTENT : (j + 1) * EXTENT] for j in range(count)]


def sublanes_of(line):
    return lax.broadcasted_iota(jnp.int32, line.shape, 0)


def gather_points(lines, k):
    rows = sublanes_of(lines[0])
    points = pltpu.roll(lines[0], (EXTENT - k) % EXTENT, 0) if k else lines[0]
    for j, line in enumerate(lines):
        if j:
            moved = pltpu.roll(line, (j - k) % EXTENT, 0) if (j - k) % EXTENT else line
            points = jnp.where(rows == j, moved, points)
    return points


def point_at(points, j, k):
    return pltpu.roll(points, (k - j) % EXTENT, 0) if (k - j) % EXTENT else points


def lower_of(values):
    lines = lines_of(values, EXTENT)
    lines = [lines[0] + lane_backward(lines[ORDER], EZ, EY)] + lines[1:ORDER]
    back = lane_backward(gather_points(lines, ORDER), 1, EZ)
    rows = sublanes_of(back)
    return [
        jnp.where(rows == 0, line + point_at(back, j, 0), line) for j, line in enumerate(lines)
    ]


def assembled_of(values):
    lines = lines_of(values, EXTENT)
    low = lines[0] + lane_backward(lines[ORDER], EZ, EY)
    high = lines[ORDER] + lane_forward(lines[0], EZ, EY)
    lines = [low] + lines[1:ORDER] + [high]
    back = lane_backward(gather_points(lines, ORDER), 1, EZ)
    ahead = lane_forward(gather_points(lines, 0), 1, EZ)
    rows = sublanes_of(back)
    return [
        jnp.where(
            rows == 0,
            line + point_at(back, j, 0),
            jnp.where(rows == ORDER, line + point_at(ahead, j, ORDER), line),
        )
        for j, line in enumerate(lines)
    ]


def spread_of(lines):
    ahead = lane_forward(gather_points(lines, 0), 1, EZ)
    rows = sublanes_of(ahead)
    lines = [
        jnp.where(rows == ORDER, point_at(ahead, j, ORDER), line) for j, line in enumerate(lines)
    ]
    return lines + [lane_forward(lines[0], EZ, EY)]


def plane_of(lines):
    return jnp.concatenate(lines, axis=0)


def store_sent(ref, lines):
    tail = lines[ORDER - 1]
    rows = sublanes_of(tail)
    for j in range(ORDER - 1):
        ref[j * EXTENT : (j + 1) * EXTENT] = jnp.where(
            rows == ORDER, point_at(tail, j + 1, ORDER), lines[j]
        )
    ref[TAIL:LOWER] = tail


def received(packed):
    tail = packed[pl.ds(ORDER, EXTENT, stride=EXTENT), :]
    rows = sublanes_of(tail)
    tail = jnp.where(rows == 0, packed[LOWER : LOWER + EXTENT], tail)
    return lines_of(packed[EXTENT:LOWER], ORDER - 1) + [tail]


def add_lines(one, other):
    return [a + b for a, b in zip(one, other)]


def kernel(
    count, members, groups, scalars_in, transport_in, mass_in, order_in, matrix_in, out,
    state,    scalars, transport, mass, order, matrix, load_sem, speed, bulk, middle, ahead, work, raw, joint, cross, beyond,
    mass_send, mass_recv, mass_send_sem, mass_recv_sem,
    coef_send, coef_recv, coef_send_sem, coef_recv_sem, share_send_sem, share_recv_sem,
    send, recv, send_sem, recv_sem,
):
    me, group = lax.axis_index("elem"), lax.axis_index("ens")

    def shifted(distance):
        return lax.rem(me + distance + count, count)

    def peer(distance):
        return {"ens": lax.rem(group + distance, groups)}

    barrier = pltpu.get_barrier_semaphore()
    for distance in (-2, -1, 1, 2):
        pl.semaphore_signal(
            barrier, inc=1, device_id={"elem": shifted(distance)}, device_id_type=MESH
        )
    for distance in range(1, groups):
        pl.semaphore_signal(barrier, inc=1, device_id=peer(distance), device_id_type=MESH)

    loads = [
        pltpu.make_async_copy(source, place, load_sem.at[number])
        for number, (source, place) in enumerate(
            (
                (order_in, order), (mass_in, mass), (scalars_in, scalars),
                (transport_in, transport), (matrix_in, matrix),
            )
        )
    ]
    for load in loads:
        load.start()
    loads[0].wait()

    elements = order.shape[-1]
    lanes = lax.broadcasted_iota(jnp.int32, (elements, elements), 0)
    chosen = jnp.where(order[...] == lanes, 1.0, 0.0).astype(jnp.bfloat16)
    to_brick_matrix = jnp.concatenate([chosen, chosen], axis=1)

    def to_brick(values):
        return lax.dot_general(
            jnp.concatenate(halves(values), axis=1),
            to_brick_matrix,
            (((1,), (1,)), ((), ())),
            preferred_element_type=jnp.float32,
        )

    first_side = 1 - lax.rem(me, 2)
    sides = (first_side, 1 - first_side)
    ends = (ORDER, 0)

    def target(side, distance):
        return {"elem": lax.rem(me + count + distance * (1 - 2 * side), count)}

    def mass_copies(m):
        return [
            pltpu.make_async_remote_copy(
                src_ref=mass_send.at[m, side, pl.ds(0, SENT)],
                dst_ref=mass_recv.at[m, side, pl.ds(EXTENT, SENT)],
                send_sem=mass_send_sem.at[m, side],
                recv_sem=mass_recv_sem.at[m, side],
                device_id=target(side, 1),
                device_id_type=MESH,
            )
            for side in sides
        ]

    share = 3 * PLANE // groups
    shared = pl.ds(pl.multiple_of(group * share, 8), share)

    def coef_copies():
        return [
            pltpu.make_async_remote_copy(
                src_ref=coef_send.at[side, shared],
                dst_ref=coef_recv.at[side, shared],
                send_sem=coef_send_sem.at[side],
                recv_sem=coef_recv_sem.at[side],
                device_id=target(side, 1),
                device_id_type=MESH,
            )
            for side in sides
        ]

    def share_copies():
        return [
            pltpu.make_async_remote_copy(
                src_ref=coef_recv.at[side, shared],
                dst_ref=coef_recv.at[side, shared],
                send_sem=share_send_sem.at[distance - 1, side],
                recv_sem=share_recv_sem.at[distance - 1, side],
                device_id=peer(distance),
                device_id_type=MESH,
            )
            for distance in range(1, groups)
            for side in sides
        ]

    def face_copies(slot, m, kinds):
        return [
            pltpu.make_async_remote_copy(
                src_ref=send.at[slot, m, side, kind // 2, pl.ds(0, SENT)],
                dst_ref=recv.at[slot, m, side, kind, pl.ds(EXTENT, SENT)],
                send_sem=send_sem.at[slot, m, side, kind],
                recv_sem=recv_sem.at[slot, m, side, kind],
                device_id=target(side, 2 if kind == FAR else 1),
                device_id_type=MESH,
            )
            for side in sides
            for kind in kinds
        ]

    def row_of(m, i):
        return (m * EXTENT + i) * PLANE

    def rows_of(m, i):
        return slice(row_of(m, i), row_of(m, i) + PLANE)

    def lower_rows(m, i):
        return slice(row_of(m, i), row_of(m, i) + LOWER)

    def plane_rows(i):
        return slice(i * PLANE, (i + 1) * PLANE)

    def block(values, place):
        return values[place * PLANE : (place + 1) * PLANE]

    def side_rows(m, side):
        return slice((m * 2 + side) * PLANE, (m * 2 + side + 1) * PLANE)

    loads[1].wait()
    loads[2].wait()
    outer = to_brick(
        jnp.concatenate(
            [mass[plane_rows(i), :] for i in ends]
            + [scalars[m, plane_rows(i), :] for m in range(members) for i in ends],
            axis=0,
        )
    )
    for side, i in enumerate(ends):
        lines = lower_of(block(outer, side))
        work[lower_rows(members, i), :] = plane_of(lines)
        store_sent(mass_send.at[members, side], lines)
    for m in range(members):
        for side, i in enumerate(ends):
            lines = lower_of(block(outer, side) * block(outer, 2 * (m + 1) + side))
            work[lower_rows(m, i), :] = plane_of(lines)
            store_sent(mass_send.at[m, side], lines)
    loads[3].wait()
    loads[4].wait()
    outer = to_brick(
        jnp.concatenate([transport[r, plane_rows(i), :] for r in range(3) for i in ends], axis=0)
    )
    for r in range(3):
        for side, i in enumerate(ends):
            speed[r, plane_rows(i), :] = block(outer, 2 * r + side)
            coef_send[side, plane_rows(r), :] = block(outer, 2 * r + side)
    pl.semaphore_wait(barrier, 4 + groups - 1)
    for m in (members, *range(members)):
        for copy in mass_copies(m):
            copy.start()

    for copy in coef_copies():
        copy.start()

    inner = slice(PLANE, NODES - PLANE)
    for r in range(3):
        speed[r, inner, :] = to_brick(transport[r, inner, :])
    middle[inner, :] = to_brick(mass[inner, :])
    for m in range(members):
        rows = slice(m * NODES + PLANE, (m + 1) * NODES - PLANE)
        ahead[rows, :] = to_brick(scalars[m, inner, :])
    for i in range(1, ORDER):
        weight = middle[plane_rows(i), :]
        store_assembled(work, row_of(members, i), weight)
        for m in range(members):
            store_assembled(work, row_of(m, i), weight * ahead[rows_of(m, i), :])

    def begin(m, i):
        state[0, rows_of(m, i), :] = work[rows_of(m, i), :] * work[rows_of(members, i), :]

    def scale(i):
        inverse = 1.0 / work[rows_of(members, i), :]
        work[rows_of(members, i), :] = inverse
        for r in range(3):
            speed[r, plane_rows(i), :] = speed[r, plane_rows(i), :] * (-time_step * inverse)

    for i in range(1, ORDER):
        scale(i)
        store_assembled(bulk, i * PLANE, speed[0, plane_rows(i), :])
        for m in range(members):
            begin(m, i)

    def take_masses(m):
        for copy in mass_copies(m):
            copy.wait()
        for side, i in enumerate((0, ORDER)):
            own = lines_of(work[lower_rows(m, i), :], ORDER)
            lines = add_lines(own, received(mass_recv.at[m, side]))
            work[rows_of(m, i), :] = plane_of(spread_of(lines))

    take_masses(members)
    for i in (0, ORDER):
        scale(i)
        bulk[plane_rows(i), :] = plane_of(assembled_of(speed[0, plane_rows(i), :]))

    derivative = gll_derivative(ORDER)
    half = EXTENT // 2

    def inside_of(planes):
        stacked = []
        for values in planes:
            high, low = halves(values)
            stacked.append(jnp.concatenate([high, low, high], axis=0))
        return jnp.dot(
            matrix[...], jnp.concatenate(stacked, axis=1), preferred_element_type=jnp.float32
        )

    def pair(plane, a):
        even = odd = None
        for i in range(half):
            one, other = plane(i), plane(ORDER - i)
            plus = float(derivative[a, i] + derivative[a, ORDER - i]) * 0.5
            minus = float(derivative[a, i] - derivative[a, ORDER - i]) * 0.5
            even_term = plus * (one + other)
            odd_term = minus * (one - other)
            even = even_term if even is None else even + even_term
            odd = odd_term if odd is None else odd + odd_term
        inside = inside_of([plane(a), plane(ORDER - a)])
        for place, (i, across) in enumerate(((a, odd + even), (ORDER - a, odd - even))):
            columns = slice(place * elements, (place + 1) * elements)
            yield i, (
                speed[0, plane_rows(i), :] * across
                + speed[1, plane_rows(i), :] * inside[:PLANE, columns]
                + speed[2, plane_rows(i), :] * inside[PLANE:, columns]
            )

    def reaches(slot):
        return jnp.where(slot == 0, 0.25, 0.5), jnp.where(slot == 0, 1.0 / 3.0, 1.0)

    def first_faces(index, m):
        slot = lax.rem(index, 2)
        for i, value in pair(lambda n: state[slot, rows_of(m, n), :], 0):
            lines = lower_of(value)
            store_sent(send.at[slot, m, ends.index(i), 0], lines)
            work[rows_of(m, i), :] = plane_of(spread_of(lines))
        for copy in face_copies(slot, m, (NEAR,)):
            copy.start()

    def first_inner(index, m):
        slot = lax.rem(index, 2)
        reach, _ = reaches(slot)
        for i in ends:
            middle[rows_of(m, i), :] = state[0, rows_of(m, i), :] + reach * work[rows_of(m, i), :]
        for a in range(1, half):
            for i, value in pair(lambda n: state[slot, rows_of(m, n), :], a):
                store_assembled(work, row_of(m, i), value)
                middle[rows_of(m, i), :] = (
                    state[0, rows_of(m, i), :] + reach * work[rows_of(m, i), :]
                )
        for side, i in enumerate(ends):
            across = None
            for n in range(EXTENT):
                if n != i:
                    term = float(derivative[i, n]) * middle[rows_of(m, n), :]
                    across = term if across is None else across + term
            value = bulk[plane_rows(i), :] * across
            raw[side_rows(m, side), :] = value
            store_sent(send.at[slot, m, side, 1], lines_of(value, ORDER))
        for copy in face_copies(slot, m, (NEXT, FAR)):
            copy.start()

    def second_ahead(index, m):
        _, reach = reaches(lax.rem(index, 2))
        for a in range(1, half):
            for i, value in pair(lambda n: middle[rows_of(m, n), :], a):
                store_assembled(work, row_of(m, i), value)
                ahead[rows_of(m, i), :] = (
                    state[0, rows_of(m, i), :] + reach * work[rows_of(m, i), :]
                )

    def second(index, m):
        slot = lax.rem(index, 2)
        reach, final_reach = reaches(slot)
        for copy in face_copies(slot, m, (NEAR,)):
            copy.wait()
        planes = (0, ORDER)

        def taken(side, kind):
            return spread_of(received(recv.at[slot, m, side, kind]))

        deltas = [reach * plane_of(taken(side, NEAR)) for side in range(2)]
        faces = [middle[rows_of(m, i), :] + deltas[side] for side, i in enumerate(planes)]
        inside = inside_of(faces)
        for side, i in enumerate(planes):
            columns = slice(side * elements, (side + 1) * elements)
            within_plane = assembled_of(
                joint[side, 1] * inside[:PLANE, columns]
                + joint[side, 2] * inside[PLANE:, columns]
            )
            total = (
                plane_of(within_plane)
                + joint[side, 0] * faces[side]
                + cross[side] * deltas[1 - side]
                + raw[side_rows(m, 1 - side), :]
            )
            work[rows_of(m, i), :] = state[0, rows_of(m, i), :] + final_reach * total
        low, high = (final_reach * delta for delta in deltas)
        for i in range(1, ORDER):
            across = float(derivative[i, 0]) * low + float(derivative[i, ORDER]) * high
            state[1 - slot, rows_of(m, i), :] = (
                ahead[rows_of(m, i), :] + bulk[plane_rows(i), :] * across
            )
        for copy in face_copies(slot, m, (NEXT, FAR)):
            copy.wait()
        for side, i in enumerate(planes):
            lines = [
                final_reach * (after + weight * (reach * away))
                for after, weight, away in zip(
                    received(recv.at[slot, m, side, NEXT]),
                    lines_of(beyond[side], ORDER),
                    received(recv.at[slot, m, side, FAR]),
                )
            ]
            state[1 - slot, rows_of(m, i), :] = work[rows_of(m, i), :] + plane_of(spread_of(lines))

    for m in range(members):
        take_masses(m)
        begin(m, 0)
        begin(m, ORDER)
        first_faces(0, m)
        first_inner(0, m)
        if m == 0:
            for copy in coef_copies():
                copy.wait()
            for copy in share_copies():
                copy.start()

    for m in range(members):
        second_ahead(0, m)
    for copy in share_copies():
        copy.wait()
    for side, i in enumerate((0, ORDER)):
        inverse = -time_step * work[rows_of(members, i), :]
        theirs = plane_of(assembled_of(coef_recv[side, plane_rows(0), :] * inverse))
        ours = bulk[plane_rows(i), :]
        joint[side, 0] = float(derivative[i, i]) * ours + (
            float(derivative[ORDER - i, ORDER - i]) * theirs
        )
        cross[side] = float(derivative[i, ORDER - i]) * ours
        beyond[side] = float(derivative[ORDER - i, i]) * theirs
        for r in (1, 2):
            joint[side, r] = speed[r, plane_rows(i), :] + coef_recv[side, plane_rows(r), :] * inverse

    def stage(index, carry):
        for m in range(members):
            second(index - 1, m)
            first_faces(index, m)
            first_inner(index, m)
        for m in range(members):
            second_ahead(index, m)
        return carry

    final = 2 * SUBSTEPS - 1
    lax.fori_loop(1, final + 1, stage, 0)
    for m in range(members):
        second(final, m)
        out[m, :, :] = jnp.dot(
            jnp.concatenate(halves(state[0, m * NODES : (m + 1) * NODES, :]), axis=1),
            jnp.concatenate([chosen, chosen], axis=0),
            preferred_element_type=jnp.float32,
        )


def store_kernel(result, out, store_sem):
    copy = pltpu.make_async_copy(result, out, store_sem)
    copy.start()
    copy.wait()


def per_device(scalars, transport, mass, element_order):
    members, nodes, elements = scalars.shape
    count, groups = lax.axis_size("elem"), lax.axis_size("ens")
    whole = pl.BlockSpec(memory_space=pltpu.VMEM)
    matrix = jnp.asarray(split_matrix())

    def floats(*shape):
        return pltpu.VMEM((*shape, elements), jnp.float32)

    def semaphores(*shape):
        return pltpu.SemaphoreType.DMA(shape)

    result = pl.pallas_call(
        functools.partial(kernel, count, members, groups),
        out_shape=floats(members, nodes),
        in_specs=[pl.BlockSpec(memory_space=pl.ANY)] * 5,
        out_specs=whole,
        scratch_shapes=[
            floats(2, members * nodes),
            floats(members, nodes),
            floats(3, nodes),
            floats(nodes),
            pltpu.VMEM(element_order.shape, jnp.int32),
            pltpu.VMEM(matrix.shape, matrix.dtype),
            semaphores(5),
            floats(3, nodes),
            floats(nodes),
            floats(members * nodes),
            floats(members * nodes),
            floats((members + 1) * nodes),
            floats(members * 2 * PLANE),
            floats(2, 3, PLANE),
            floats(2, PLANE),
            floats(2, PLANE),
            floats(members + 1, 2, PLANE),
            floats(members + 1, 2, PLANE),
            semaphores(members + 1, 2),
            semaphores(members + 1, 2),
            floats(2, 3 * PLANE),
            floats(2, 3 * PLANE),
            semaphores(2),
            semaphores(2),
            semaphores(groups - 1, 2),
            semaphores(groups - 1, 2),
            floats(2, members, 2, 2, PLANE),
            floats(2, members, 2, 3, PLANE),
            semaphores(2, members, 2, 3),
            semaphores(2, members, 2, 3),
        ],
        compiler_params=pltpu.CompilerParams(collective_id=0, has_side_effects=True),
    )(scalars, transport, mass, element_order, matrix)
    return pl.pallas_call(
        store_kernel,
        out_shape=jax.ShapeDtypeStruct(scalars.shape, jnp.float32),
        in_specs=[whole],
        out_specs=pl.BlockSpec(memory_space=pl.ANY),
        scratch_shapes=[pltpu.SemaphoreType.DMA],
    )(pltpu.with_memory_space_constraint(result, pltpu.VMEM))


def solution(mesh):
    in_specs = (P("ens", None, "elem"), P(None, None, "elem"), P(None, "elem"), P("elem", None))
    out_specs = P("ens", None, "elem")
    return jax.shard_map(
        per_device, mesh=mesh, in_specs=in_specs, out_specs=out_specs, check_vma=False
    )
```

```python
import functools

import jax
import jax.numpy as jnp
import numpy as np
from jax import lax
from jax.experimental import pallas as pl
from jax.experimental.pallas import tpu as pltpu
from jax.sharding import PartitionSpec as P

ORDER = 7
SUBSTEPS = 2
EX = 1
EY = 8
EZ = 16
EXTENT = ORDER + 1
PLANE = EXTENT * EXTENT
NODES = EXTENT * PLANE
MESH = pl.DeviceIdType.MESH
NEAR, FAR, NEXT = 0, 1, 2


time_step = 0.015


def legendre_table(points, degree):
    table = np.zeros((points.shape[0], degree + 1))
    table[:, 0] = 1.0
    table[:, 1] = points
    for level in range(2, degree + 1):
        table[:, level] = (
            (2 * level - 1) * points * table[:, level - 1] - (level - 1) * table[:, level - 2]
        ) / level
    return table


def gll_derivative(degree):
    extent = degree + 1
    points = np.cos(np.pi * np.arange(extent) / degree)
    for sweep in range(60):
        table = legendre_table(points, degree)
        points = points - (points * table[:, degree] - table[:, degree - 1]) / (
            extent * table[:, degree]
        )
    points = points[::-1].copy()
    values = legendre_table(points, degree)[:, degree]
    matrix = np.zeros((extent, extent))
    for target in range(extent):
        for source in range(extent):
            if target != source:
                matrix[target, source] = values[target] / (
                    values[source] * (points[target] - points[source])
                )
    matrix[0, 0] = -degree * (degree + 1) / 4.0
    matrix[extent - 1, extent - 1] = degree * (degree + 1) / 4.0
    return matrix


def split_matrix():
    derivative = gll_derivative(ORDER).astype(np.float32)
    eye = np.eye(EXTENT, dtype=np.float32)
    full = np.concatenate([np.kron(derivative, eye), np.kron(eye, derivative)], axis=0)
    high = full.astype(jnp.bfloat16)
    low = (full - high.astype(np.float32)).astype(jnp.bfloat16)
    return np.concatenate([high, high, low], axis=1)


def halves(values):
    high = values.astype(jnp.bfloat16)
    low = (values - high.astype(jnp.float32)).astype(jnp.bfloat16)
    return high, low


def lane_forward(values, stride, length):
    total = values.shape[-1]
    near = pltpu.roll(values, total - stride, 1)
    if stride * length == total:
        return near
    coords = lax.broadcasted_iota(jnp.int32, values.shape, 1) // stride % length
    return jnp.where(coords < length - 1, near, pltpu.roll(values, stride * (length - 1), 1))


def lane_backward(values, stride, length):
    total = values.shape[-1]
    near = pltpu.roll(values, stride, 1)
    if stride * length == total:
        return near
    coords = lax.broadcasted_iota(jnp.int32, values.shape, 1) // stride % length
    return jnp.where(coords > 0, near, pltpu.roll(values, total - stride * (length - 1), 1))


def store_assembled(ref, row, values):
    low, high = values[:EXTENT], values[PLANE - EXTENT :]
    ref[row : row + EXTENT] = low + lane_backward(high, EZ, EY)
    ref[row + EXTENT : row + PLANE - EXTENT] = values[EXTENT : PLANE - EXTENT]
    ref[row + PLANE - EXTENT : row + PLANE] = high + lane_forward(low, EZ, EY)
    first = pl.ds(row, EXTENT, stride=EXTENT)
    last = pl.ds(row + ORDER, EXTENT, stride=EXTENT)
    k_low = ref[first, :]
    k_high = ref[last, :]
    ref[first, :] = k_low + lane_backward(k_high, 1, EZ)
    ref[last, :] = k_high + lane_forward(k_low, 1, EZ)


LOWER = PLANE - EXTENT
SENT = ORDER * ORDER
TAIL = LOWER - EXTENT


def lines_of(values, count):
    return [values[j * EXTENT : (j + 1) * EXTENT] for j in range(count)]


def sublanes_of(line):
    return lax.broadcasted_iota(jnp.int32, line.shape, 0)


def gather_points(lines, k):
    rows = sublanes_of(lines[0])
    points = pltpu.roll(lines[0], (EXTENT - k) % EXTENT, 0) if k else lines[0]
    for j, line in enumerate(lines):
        if j:
            moved = pltpu.roll(line, (j - k) % EXTENT, 0) if (j - k) % EXTENT else line
            points = jnp.where(rows == j, moved, points)
    return points


def point_at(points, j, k):
    return pltpu.roll(points, (k - j) % EXTENT, 0) if (k - j) % EXTENT else points


def lower_of(values):
    lines = lines_of(values, EXTENT)
    lines = [lines[0] + lane_backward(lines[ORDER], EZ, EY)] + lines[1:ORDER]
    back = lane_backward(gather_points(lines, ORDER), 1, EZ)
    rows = sublanes_of(back)
    return [
        jnp.where(rows == 0, line + point_at(back, j, 0), line) for j, line in enumerate(lines)
    ]


def assembled_of(values):
    lines = lines_of(values, EXTENT)
    low = lines[0] + lane_backward(lines[ORDER], EZ, EY)
    high = lines[ORDER] + lane_forward(lines[0], EZ, EY)
    lines = [low] + lines[1:ORDER] + [high]
    back = lane_backward(gather_points(lines, ORDER), 1, EZ)
    ahead = lane_forward(gather_points(lines, 0), 1, EZ)
    rows = sublanes_of(back)
    return [
        jnp.where(
            rows == 0,
            line + point_at(back, j, 0),
            jnp.where(rows == ORDER, line + point_at(ahead, j, ORDER), line),
        )
        for j, line in enumerate(lines)
    ]


def spread_of(lines):
    ahead = lane_forward(gather_points(lines, 0), 1, EZ)
    rows = sublanes_of(ahead)
    lines = [
        jnp.where(rows == ORDER, point_at(ahead, j, ORDER), line) for j, line in enumerate(lines)
    ]
    return lines + [lane_forward(lines[0], EZ, EY)]


def plane_of(lines):
    return jnp.concatenate(lines, axis=0)


def store_sent(ref, lines):
    tail = lines[ORDER - 1]
    rows = sublanes_of(tail)
    for j in range(ORDER - 1):
        ref[j * EXTENT : (j + 1) * EXTENT] = jnp.where(
            rows == ORDER, point_at(tail, j + 1, ORDER), lines[j]
        )
    ref[TAIL:LOWER] = tail


def received(packed):
    tail = packed[pl.ds(ORDER, EXTENT, stride=EXTENT), :]
    rows = sublanes_of(tail)
    tail = jnp.where(rows == 0, packed[LOWER : LOWER + EXTENT], tail)
    return lines_of(packed[EXTENT:LOWER], ORDER - 1) + [tail]


def add_lines(one, other):
    return [a + b for a, b in zip(one, other)]


def kernel(
    count, members, groups, scalars_in, transport_in, mass_in, order_in, matrix_in, out,
    state,    scalars, transport, mass, order, matrix, load_sem, speed, bulk, middle, ahead, work, raw, joint, cross, beyond,
    mass_send, mass_recv, mass_send_sem, mass_recv_sem,
    coef_send, coef_recv, coef_send_sem, coef_recv_sem, share_send_sem, share_recv_sem,
    send, recv, send_sem, recv_sem,
):
    me, group = lax.axis_index("elem"), lax.axis_index("ens")

    def shifted(distance):
        return lax.rem(me + distance + count, count)

    def peer(distance):
        return {"ens": lax.rem(group + distance, groups)}

    barrier = pltpu.get_barrier_semaphore()
    for distance in (-2, -1, 1, 2):
        pl.semaphore_signal(
            barrier, inc=1, device_id={"elem": shifted(distance)}, device_id_type=MESH
        )
    for distance in range(1, groups):
        pl.semaphore_signal(barrier, inc=1, device_id=peer(distance), device_id_type=MESH)

    loads = [
        pltpu.make_async_copy(source, place, load_sem.at[number])
        for number, (source, place) in enumerate(
            (
                (order_in, order), (mass_in, mass), (scalars_in, scalars),
                (transport_in, transport), (matrix_in, matrix),
            )
        )
    ]
    for load in loads:
        load.start()
    loads[0].wait()

    elements = order.shape[-1]
    lanes = lax.broadcasted_iota(jnp.int32, (elements, elements), 0)
    chosen = jnp.where(order[...] == lanes, 1.0, 0.0).astype(jnp.bfloat16)
    to_brick_matrix = jnp.concatenate([chosen, chosen], axis=1)

    def to_brick(values):
        return lax.dot_general(
            jnp.concatenate(halves(values), axis=1),
            to_brick_matrix,
            (((1,), (1,)), ((), ())),
            preferred_element_type=jnp.float32,
        )

    first_side = 1 - lax.rem(me, 2)
    sides = (first_side, 1 - first_side)
    ends = (ORDER, 0)

    def target(side, distance):
        return {"elem": lax.rem(me + count + distance * (1 - 2 * side), count)}

    def mass_copies(m):
        return [
            pltpu.make_async_remote_copy(
                src_ref=mass_send.at[m, side, pl.ds(0, SENT)],
                dst_ref=mass_recv.at[m, side, pl.ds(EXTENT, SENT)],
                send_sem=mass_send_sem.at[m, side],
                recv_sem=mass_recv_sem.at[m, side],
                device_id=target(side, 1),
                device_id_type=MESH,
            )
            for side in sides
        ]

    share = 3 * PLANE // groups
    shared = pl.ds(pl.multiple_of(group * share, 8), share)

    def coef_copies():
        return [
            pltpu.make_async_remote_copy(
                src_ref=coef_send.at[side, shared],
                dst_ref=coef_recv.at[side, shared],
                send_sem=coef_send_sem.at[side],
                recv_sem=coef_recv_sem.at[side],
                device_id=target(side, 1),
                device_id_type=MESH,
            )
            for side in sides
        ]

    def share_copies(places):
        return [
            pltpu.make_async_remote_copy(
                src_ref=coef_recv.at[side, shared],
                dst_ref=coef_recv.at[side, shared],
                send_sem=share_send_sem.at[distance - 1, side],
                recv_sem=share_recv_sem.at[distance - 1, side],
                device_id=peer(distance),
                device_id_type=MESH,
            )
            for distance in range(1, groups)
            for side in (sides[place] for place in places)
        ]

    def face_copies(slot, m, kinds):
        return [
            pltpu.make_async_remote_copy(
                src_ref=send.at[slot, m, side, kind // 2, pl.ds(0, SENT)],
                dst_ref=recv.at[slot, m, side, kind, pl.ds(EXTENT, SENT)],
                send_sem=send_sem.at[slot, m, side, kind],
                recv_sem=recv_sem.at[slot, m, side, kind],
                device_id=target(side, 2 if kind == FAR else 1),
                device_id_type=MESH,
            )
            for side in sides
            for kind in kinds
        ]

    def row_of(m, i):
        return (m * EXTENT + i) * PLANE

    def rows_of(m, i):
        return slice(row_of(m, i), row_of(m, i) + PLANE)

    def lower_rows(m, i):
        return slice(row_of(m, i), row_of(m, i) + LOWER)

    def plane_rows(i):
        return slice(i * PLANE, (i + 1) * PLANE)

    def block(values, place):
        return values[place * PLANE : (place + 1) * PLANE]

    def side_rows(m, side):
        return slice((m * 2 + side) * PLANE, (m * 2 + side + 1) * PLANE)

    loads[1].wait()
    loads[2].wait()
    outer = to_brick(
        jnp.concatenate(
            [mass[plane_rows(i), :] for i in ends]
            + [scalars[m, plane_rows(i), :] for m in range(members) for i in ends],
            axis=0,
        )
    )
    for side, i in enumerate(ends):
        lines = lower_of(block(outer, side))
        work[lower_rows(members, i), :] = plane_of(lines)
        store_sent(mass_send.at[members, side], lines)
    for m in range(members):
        for side, i in enumerate(ends):
            lines = lower_of(block(outer, side) * block(outer, 2 * (m + 1) + side))
            work[lower_rows(m, i), :] = plane_of(lines)
            store_sent(mass_send.at[m, side], lines)
    loads[3].wait()
    loads[4].wait()
    outer = to_brick(
        jnp.concatenate([transport[r, plane_rows(i), :] for r in range(3) for i in ends], axis=0)
    )
    for r in range(3):
        for side, i in enumerate(ends):
            speed[r, plane_rows(i), :] = block(outer, 2 * r + side)
            coef_send[side, plane_rows(r), :] = block(outer, 2 * r + side)
    pl.semaphore_wait(barrier, 4 + groups - 1)
    for m in (members, *range(members)):
        for copy in mass_copies(m):
            copy.start()

    for copy in coef_copies():
        copy.start()

    inner = slice(PLANE, NODES - PLANE)
    for r in range(3):
        speed[r, inner, :] = to_brick(transport[r, inner, :])
    middle[inner, :] = to_brick(mass[inner, :])
    for m in range(members):
        rows = slice(m * NODES + PLANE, (m + 1) * NODES - PLANE)
        ahead[rows, :] = to_brick(scalars[m, inner, :])
    for i in range(1, ORDER):
        weight = middle[plane_rows(i), :]
        store_assembled(work, row_of(members, i), weight)
        for m in range(members):
            store_assembled(work, row_of(m, i), weight * ahead[rows_of(m, i), :])

    def begin(m, i):
        state[0, rows_of(m, i), :] = work[rows_of(m, i), :] * work[rows_of(members, i), :]

    def scale(i):
        inverse = 1.0 / work[rows_of(members, i), :]
        work[rows_of(members, i), :] = inverse
        for r in range(3):
            speed[r, plane_rows(i), :] = speed[r, plane_rows(i), :] * (-time_step * inverse)

    for i in range(1, ORDER):
        scale(i)
        store_assembled(bulk, i * PLANE, speed[0, plane_rows(i), :])
        for m in range(members):
            begin(m, i)

    def take_masses(m):
        for copy in mass_copies(m):
            copy.wait()
        for side, i in enumerate((0, ORDER)):
            own = lines_of(work[lower_rows(m, i), :], ORDER)
            lines = add_lines(own, received(mass_recv.at[m, side]))
            work[rows_of(m, i), :] = plane_of(spread_of(lines))

    take_masses(members)
    for i in (0, ORDER):
        scale(i)
        bulk[plane_rows(i), :] = plane_of(assembled_of(speed[0, plane_rows(i), :]))

    derivative = gll_derivative(ORDER)
    half = EXTENT // 2

    def inside_of(planes):
        stacked = []
        for values in planes:
            high, low = halves(values)
            stacked.append(jnp.concatenate([high, low, high], axis=0))
        return jnp.dot(
            matrix[...], jnp.concatenate(stacked, axis=1), preferred_element_type=jnp.float32
        )

    def pair(plane, a):
        even = odd = None
        for i in range(half):
            one, other = plane(i), plane(ORDER - i)
            plus = float(derivative[a, i] + derivative[a, ORDER - i]) * 0.5
            minus = float(derivative[a, i] - derivative[a, ORDER - i]) * 0.5
            even_term = plus * (one + other)
            odd_term = minus * (one - other)
            even = even_term if even is None else even + even_term
            odd = odd_term if odd is None else odd + odd_term
        inside = inside_of([plane(a), plane(ORDER - a)])
        for place, (i, across) in enumerate(((a, odd + even), (ORDER - a, odd - even))):
            columns = slice(place * elements, (place + 1) * elements)
            yield i, (
                speed[0, plane_rows(i), :] * across
                + speed[1, plane_rows(i), :] * inside[:PLANE, columns]
                + speed[2, plane_rows(i), :] * inside[PLANE:, columns]
            )

    def reaches(slot):
        return jnp.where(slot == 0, 0.25, 0.5), jnp.where(slot == 0, 1.0 / 3.0, 1.0)

    def first_faces(index, m):
        slot = lax.rem(index, 2)
        for i, value in pair(lambda n: state[slot, rows_of(m, n), :], 0):
            lines = lower_of(value)
            store_sent(send.at[slot, m, ends.index(i), 0], lines)
            work[rows_of(m, i), :] = plane_of(spread_of(lines))
        for copy in face_copies(slot, m, (NEAR,)):
            copy.start()

    def first_inner(index, m):
        slot = lax.rem(index, 2)
        reach, _ = reaches(slot)
        for i in ends:
            middle[rows_of(m, i), :] = state[0, rows_of(m, i), :] + reach * work[rows_of(m, i), :]
        for a in range(1, half):
            for i, value in pair(lambda n: state[slot, rows_of(m, n), :], a):
                store_assembled(work, row_of(m, i), value)
                middle[rows_of(m, i), :] = (
                    state[0, rows_of(m, i), :] + reach * work[rows_of(m, i), :]
                )
        for side, i in enumerate(ends):
            across = None
            for n in range(EXTENT):
                if n != i:
                    term = float(derivative[i, n]) * middle[rows_of(m, n), :]
                    across = term if across is None else across + term
            value = bulk[plane_rows(i), :] * across
            raw[side_rows(m, side), :] = value
            store_sent(send.at[slot, m, side, 1], lines_of(value, ORDER))
        for copy in face_copies(slot, m, (NEXT, FAR)):
            copy.start()

    def second_ahead(index, m):
        _, reach = reaches(lax.rem(index, 2))
        for a in range(1, half):
            for i, value in pair(lambda n: middle[rows_of(m, n), :], a):
                store_assembled(work, row_of(m, i), value)
                ahead[rows_of(m, i), :] = (
                    state[0, rows_of(m, i), :] + reach * work[rows_of(m, i), :]
                )

    def second(index, m):
        slot = lax.rem(index, 2)
        reach, final_reach = reaches(slot)
        for copy in face_copies(slot, m, (NEAR,)):
            copy.wait()
        planes = (0, ORDER)

        def taken(side, kind):
            return spread_of(received(recv.at[slot, m, side, kind]))

        deltas = [reach * plane_of(taken(side, NEAR)) for side in range(2)]
        faces = [middle[rows_of(m, i), :] + deltas[side] for side, i in enumerate(planes)]
        inside = inside_of(faces)
        for side, i in enumerate(planes):
            columns = slice(side * elements, (side + 1) * elements)
            within_plane = assembled_of(
                joint[side, 1] * inside[:PLANE, columns]
                + joint[side, 2] * inside[PLANE:, columns]
            )
            total = (
                plane_of(within_plane)
                + joint[side, 0] * faces[side]
                + cross[side] * deltas[1 - side]
                + raw[side_rows(m, 1 - side), :]
            )
            work[rows_of(m, i), :] = state[0, rows_of(m, i), :] + final_reach * total
        low, high = (final_reach * delta for delta in deltas)
        for i in range(1, ORDER):
            across = float(derivative[i, 0]) * low + float(derivative[i, ORDER]) * high
            state[1 - slot, rows_of(m, i), :] = (
                ahead[rows_of(m, i), :] + bulk[plane_rows(i), :] * across
            )
        for copy in face_copies(slot, m, (NEXT, FAR)):
            copy.wait()
        for side, i in enumerate(planes):
            lines = [
                final_reach * (after + weight * (reach * away))
                for after, weight, away in zip(
                    received(recv.at[slot, m, side, NEXT]),
                    lines_of(beyond[side], ORDER),
                    received(recv.at[slot, m, side, FAR]),
                )
            ]
            state[1 - slot, rows_of(m, i), :] = work[rows_of(m, i), :] + plane_of(spread_of(lines))

    for m in range(members):
        take_masses(m)
        if m == 0:
            coef_copies()[1].wait()
            for copy in share_copies((1,)):
                copy.start()
        begin(m, 0)
        begin(m, ORDER)
        first_faces(0, m)
        first_inner(0, m)
        if m == 0:
            coef_copies()[0].wait()
            for copy in share_copies((0,)):
                copy.start()

    for m in range(members):
        second_ahead(0, m)
    for copy in share_copies((0, 1)):
        copy.wait()
    for side, i in enumerate((0, ORDER)):
        inverse = -time_step * work[rows_of(members, i), :]
        theirs = plane_of(assembled_of(coef_recv[side, plane_rows(0), :] * inverse))
        ours = bulk[plane_rows(i), :]
        joint[side, 0] = float(derivative[i, i]) * ours + (
            float(derivative[ORDER - i, ORDER - i]) * theirs
        )
        cross[side] = float(derivative[i, ORDER - i]) * ours
        beyond[side] = float(derivative[ORDER - i, i]) * theirs
        for r in (1, 2):
            joint[side, r] = speed[r, plane_rows(i), :] + coef_recv[side, plane_rows(r), :] * inverse

    def stage(index, carry):
        for m in range(members):
            second(index - 1, m)
            first_faces(index, m)
            first_inner(index, m)
        for m in range(members):
            second_ahead(index, m)
        return carry

    final = 2 * SUBSTEPS - 1
    lax.fori_loop(1, final + 1, stage, 0)
    for m in range(members):
        second(final, m)
        out[m, :, :] = jnp.dot(
            jnp.concatenate(halves(state[0, m * NODES : (m + 1) * NODES, :]), axis=1),
            jnp.concatenate([chosen, chosen], axis=0),
            preferred_element_type=jnp.float32,
        )


def store_kernel(result, out, store_sem):
    copy = pltpu.make_async_copy(result, out, store_sem)
    copy.start()
    copy.wait()


def per_device(scalars, transport, mass, element_order):
    members, nodes, elements = scalars.shape
    count, groups = lax.axis_size("elem"), lax.axis_size("ens")
    whole = pl.BlockSpec(memory_space=pltpu.VMEM)
    matrix = jnp.asarray(split_matrix())

    def floats(*shape):
        return pltpu.VMEM((*shape, elements), jnp.float32)

    def semaphores(*shape):
        return pltpu.SemaphoreType.DMA(shape)

    result = pl.pallas_call(
        functools.partial(kernel, count, members, groups),
        out_shape=floats(members, nodes),
        in_specs=[pl.BlockSpec(memory_space=pl.ANY)] * 5,
        out_specs=whole,
        scratch_shapes=[
            floats(2, members * nodes),
            floats(members, nodes),
            floats(3, nodes),
            floats(nodes),
            pltpu.VMEM(element_order.shape, jnp.int32),
            pltpu.VMEM(matrix.shape, matrix.dtype),
            semaphores(5),
            floats(3, nodes),
            floats(nodes),
            floats(members * nodes),
            floats(members * nodes),
            floats((members + 1) * nodes),
            floats(members * 2 * PLANE),
            floats(2, 3, PLANE),
            floats(2, PLANE),
            floats(2, PLANE),
            floats(members + 1, 2, PLANE),
            floats(members + 1, 2, PLANE),
            semaphores(members + 1, 2),
            semaphores(members + 1, 2),
            floats(2, 3 * PLANE),
            floats(2, 3 * PLANE),
            semaphores(2),
            semaphores(2),
            semaphores(groups - 1, 2),
            semaphores(groups - 1, 2),
            floats(2, members, 2, 2, PLANE),
            floats(2, members, 2, 3, PLANE),
            semaphores(2, members, 2, 3),
            semaphores(2, members, 2, 3),
        ],
        compiler_params=pltpu.CompilerParams(collective_id=0, has_side_effects=True),
    )(scalars, transport, mass, element_order, matrix)
    return pl.pallas_call(
        store_kernel,
        out_shape=jax.ShapeDtypeStruct(scalars.shape, jnp.float32),
        in_specs=[whole],
        out_specs=pl.BlockSpec(memory_space=pl.ANY),
        scratch_shapes=[pltpu.SemaphoreType.DMA],
    )(pltpu.with_memory_space_constraint(result, pltpu.VMEM))


def solution(mesh):
    in_specs = (P("ens", None, "elem"), P(None, None, "elem"), P(None, "elem"), P("elem", None))
    out_specs = P("ens", None, "elem")
    return jax.shard_map(
        per_device, mesh=mesh, in_specs=in_specs, out_specs=out_specs, check_vma=False
    )
```
